512 devices in a mesh: dp: 32 (over x, z), heads: 16 (over y, core).
Axes of the slice: x: 4, y: 8, z: 8, core: 2. Of those that a mesh axis runs over, the one named last changes fastest.
Arguments:
- queries: bfloat16 [8, 8192, 4096], P(None, ('dp', 'heads')), may hold values from -6 to 6
- keys: bfloat16 [8, 8192, 2048], P(None, ('dp', 'heads')), may hold values from -6 to 6
- values: bfloat16 [8, 8192, 2048], P(None, ('dp', 'heads')), may hold values from -6 to 6
- lengths: int32 [8, 32], replicated, may hold values from 1 to 1024, 8192 in all within a row
Outputs:
- attended: bfloat16 [8, 8192, 4096], P(None, ('dp', 'heads'))
- log_norm: float32 [32, 8, 8192], P('heads', None, 'dp')
The draws below stay inside these ranges and needn't reach their ends.
Inputs may be any that keep to these rules, and one draw needn't show every extreme that they name: In each row the 32 lengths sum to 8192, and the longest is exactly 1024.
All inputs are finite; a program needn't handle non-finite values.
Results may differ from the reference program's by a relative error of at most 0.0034.
Values may be sent and summed in bfloat16 or wider, within the bound.
No kernel may reach another device: no remote copies, remote signals or barrier semaphores. Data moves between devices by JAX's collectives and lax.ppermute only.
A program may use at most 64 MiB of HBM per device.

```python
import math
import jax
import jax.numpy as jnp
import numpy as np
from jax import lax

HEAD_SIZE = 128
PACKED_ROWS = 8
DOCS = 32
VALUE_KEY_HEADS = 16
QUERY_HEADS = 32
ROW_POSITIONS = 8192
MOST = 1024


def draw_queries(key, part):
    sampled_values = jax.random.truncated_normal(jax.random.fold_in(key, 11), -6.0, 6.0, (PACKED_ROWS, ROW_POSITIONS, QUERY_HEADS * HEAD_SIZE), jnp.float32)
    return sampled_values.astype(jnp.bfloat16)


def draw_keys(key, part):
    sampled_values = jax.random.truncated_normal(jax.random.fold_in(key, 23), -6.0, 6.0, (PACKED_ROWS, ROW_POSITIONS, VALUE_KEY_HEADS * HEAD_SIZE), jnp.float32)
    return sampled_values.astype(jnp.bfloat16)


def block_levels(stream_key, shape, split, smallest, top_value):
    factor_of = 1.0
    for dim, shards_of in split:
        heights = jax.random.uniform(jax.random.fold_in(jax.random.fold_in(stream_key, 6), dim), (shards_of,), jnp.float32, smallest / len(split), top_value / len(split))
        factor_of = factor_of * jnp.repeat(jnp.exp(heights), shape[dim] // shards_of).reshape((-1,) + (1,) * (len(shape) - 1 - dim))
    return factor_of


def length_profile(count, total, most, lean):
    weights = [(1 << 20) // math.isqrt(standing ** lean) + 1 for standing in range(2, count + 1)]
    rest, given = total - most - (count - 1), [1] * (count - 1)
    while rest > 0:
        candidates = [i for i in range(count - 1) if given[i] < most]
        pool, remaining = sum([weights[i] for i in candidates]), rest
        for i in candidates:
            more = min(most - given[i], max(1, remaining * weights[i] // pool), rest)
            given[i] = given[i] + more
            rest = rest - more
    return np.array([most] + given)


def uneven_parts(own_key, number_of, total, reach, skew):
    if number_of == 2:
        one = jax.random.randint(own_key, (), max(1, total - reach), min(reach, total - 1) + 1)
        return jnp.stack([one, total - one])
    sizes = jnp.asarray(length_profile(number_of, total, reach, skew), jnp.int32)
    pairs = (number_of - 1) // 2
    giver, taker = sizes[1:1 + 2 * pairs:2], sizes[2:2 + 2 * pairs:2]
    room = jnp.minimum(giver - 1, reach - taker)
    moved = jax.random.randint(jax.random.fold_in(own_key, 1), (pairs,), 0, 1 << 20) % (room + 1)
    sizes = sizes.at[1:1 + 2 * pairs:2].set(giver - moved).at[2:2 + 2 * pairs:2].set(taker + moved)
    return sizes[jax.random.permutation(jax.random.fold_in(own_key, 2), number_of)]


def normal_values(stream_key, extent, width, bound, split=(), kind=jnp.bfloat16):
    loudness = block_levels(stream_key, extent, split, -0.22, 0.18) if split else 1.0
    array = jax.random.normal(stream_key, extent, jnp.float32) * width * loudness
    return jnp.minimum(jnp.maximum(array, -bound), bound).astype(kind)


def setup_inputs(seed: int = 0) -> dict:
    streams_of = jax.random.split(jax.random.key(seed), 5)
    queries = draw_queries(jax.random.fold_in(streams_of[4], 71), 0)
    keys = draw_keys(jax.random.fold_in(streams_of[4], 71), 0)
    values = normal_values(streams_of[2], (PACKED_ROWS, ROW_POSITIONS, VALUE_KEY_HEADS * HEAD_SIZE), 1.0, 6.0, ((1, 512),))
    lengths = jax.vmap(lambda own: uneven_parts(own, DOCS, ROW_POSITIONS, MOST, 2))(jax.random.split(streams_of[3], PACKED_ROWS)).reshape((PACKED_ROWS, DOCS)).astype(jnp.int32)
    return {"queries": queries, "keys": keys, "values": values, "lengths": lengths}


def reference(queries, keys, values, lengths):
    row_count, seq_len, q_width = queries.shape
    heads_q = q_width // HEAD_SIZE
    heads_kv = keys.shape[2] // HEAD_SIZE
    per_group = heads_q // heads_kv
    query_block = min(512, seq_len)
    key_span = min(seq_len, query_block + MOST)
    block_count = seq_len // query_block
    doc_ends = jnp.cumsum(lengths, axis=1).astype(jnp.int32)
    positions = jnp.arange(seq_len, dtype=jnp.int32)
    doc_ids = jnp.sum((doc_ends[:, None, :] <= positions[None, :, None]).astype(jnp.int32), axis=-1)

    def attend_block(flat_index):
        row_index = (flat_index // block_count).astype(jnp.int32)
        query_first = ((flat_index % block_count) * query_block).astype(jnp.int32)
        key_first = jnp.clip(query_first - MOST, 0, seq_len - key_span).astype(jnp.int32)
        zero = jnp.zeros((), jnp.int32)
        query_rows = lax.dynamic_slice(queries, (row_index, query_first, zero), (1, query_block, q_width))[0]
        key_rows = lax.dynamic_slice(keys, (row_index, key_first, zero), (1, key_span, heads_kv * HEAD_SIZE))[0]
        value_rows = lax.dynamic_slice(values, (row_index, key_first, zero), (1, key_span, heads_kv * HEAD_SIZE))[0]
        query_heads = query_rows.reshape(query_block, heads_q, HEAD_SIZE).astype(jnp.float32)
        key_heads = jnp.repeat(key_rows.reshape(key_span, heads_kv, HEAD_SIZE), per_group, axis=1).astype(jnp.float32)
        value_heads = jnp.repeat(value_rows.reshape(key_span, heads_kv, HEAD_SIZE), per_group, axis=1).astype(jnp.float32)
        row_docs = lax.dynamic_slice(doc_ids, (row_index, zero), (1, seq_len))[0]
        query_pos = query_first + jnp.arange(query_block, dtype=jnp.int32)
        key_pos = key_first + jnp.arange(key_span, dtype=jnp.int32)
        query_doc = lax.dynamic_slice_in_dim(row_docs, query_first, query_block, 0)
        key_doc = lax.dynamic_slice_in_dim(row_docs, key_first, key_span, 0)
        visible = (query_doc[:, None] == key_doc[None, :]) & (key_pos[None, :] <= query_pos[:, None])
        scores = jnp.einsum("qhd,khd->hqk", query_heads, key_heads) * (HEAD_SIZE ** -0.5)
        masked = jnp.where(visible[None], scores, -jnp.inf)
        row_max = jnp.max(masked, axis=-1)
        weights = jnp.where(visible[None], jnp.exp(masked - row_max[..., None]), jnp.float32(0.0))
        row_sum = jnp.sum(weights, axis=-1)
        rounded = lax.optimization_barrier(weights.astype(jnp.bfloat16)).astype(jnp.float32)
        summed = jnp.einsum("hqk,khd->qhd", rounded, value_heads)
        result = (summed / jnp.transpose(row_sum)[:, :, None]).astype(jnp.bfloat16)
        log_norm = row_max + jnp.log(row_sum)
        return result.reshape(query_block, q_width), log_norm

    outputs, norms = lax.map(attend_block, jnp.arange(row_count * block_count, dtype=jnp.int32))
    attended = outputs.reshape(row_count, seq_len, q_width)
    norms = norms.reshape(row_count, block_count, heads_q, query_block)
    log_norm = jnp.transpose(norms, (2, 0, 1, 3)).reshape(heads_q, row_count, seq_len)
    return attended, log_norm
```

```python
import jax
import jax.numpy as jnp
from jax import lax
from jax.experimental import pallas as pl
from jax.experimental.pallas import tpu as pltpu
from jax.sharding import Mesh
from jax.sharding import PartitionSpec as P

HEAD = 128
ROWS = 8
KV_HEADS = 16
HALO = 1024
SPAN = 2048
TQ = 128
TK = 256
MOST_BLOCKS = 6
LOG2E = 1.4426950408889634
SCALE = HEAD ** (-0.5)
ALL = ("x", "z", "y", "c")
PLANE = ("z", "y", "c")


def pack_body(q_ref, k_ref, v_ref, out_ref):
    for h in range(KV_HEADS):
        out_ref[h, :, 0:256] = q_ref[0, :, h * 256 : (h + 1) * 256]
        out_ref[h, :, 256:384] = k_ref[0, :, h * 128 : (h + 1) * 128]
        out_ref[h, :, 384:512] = v_ref[0, :, h * 128 : (h + 1) * 128]


def pack(queries, keys, values):
    wide = lambda width: pl.BlockSpec((1, 16, width), lambda r: (r, 0, 0))
    return pl.pallas_call(
        pack_body,
        grid=(ROWS,),
        in_specs=[wide(4096), wide(2048), wide(2048)],
        out_specs=pl.BlockSpec((KV_HEADS, 16, 512), lambda r: (r, 0, 0)),
        out_shape=jax.ShapeDtypeStruct((ROWS * KV_HEADS, 16, 512), jnp.bfloat16),
        name="pack",
    )(queries, keys, values)


def unpack_body(in_ref, out_ref):
    for h in range(KV_HEADS):
        out_ref[0, :, h * 256 : (h + 1) * 256] = in_ref[h]


def unpack(parts):
    return pl.pallas_call(
        unpack_body,
        grid=(ROWS,),
        in_specs=[pl.BlockSpec((KV_HEADS, 16, 256), lambda r: (r, 0, 0))],
        out_specs=pl.BlockSpec((1, 16, 4096), lambda r: (r, 0, 0)),
        out_shape=jax.ShapeDtypeStruct((ROWS, 16, 4096), jnp.bfloat16),
        name="unpack",
    )(parts)


def attend_body(low_ref, start_ref, qkv_ref, halo_ref, out_ref, norm_ref, kv_ref, s_ref, norm_acc):
    kv_ref[0:HALO] = halo_ref[...]
    kv_ref[HALO : HALO + SPAN] = qkv_ref[:, 256:512]
    lanes = lax.broadcasted_iota(jnp.int32, (TQ, 128), 1)
    key_lane = lax.broadcasted_iota(jnp.int32, (TQ, TK), 1)
    key_row = lax.broadcasted_iota(jnp.int32, (TQ, TK), 0)
    norm_acc[...] = jnp.zeros((TQ, 128), jnp.float32)

    def block(i, carry):
        first = pl.multiple_of(i * TQ, TQ)
        q0 = qkv_ref[pl.ds(first, TQ), 0:128]
        q1 = qkv_ref[pl.ds(first, TQ), 128:256]
        both = jnp.concatenate((q0, q1), axis=0)
        start = start_ref[pl.ds(first, TQ), :]
        start = jnp.concatenate((start, start), axis=1)
        j_low = low_ref[i] // TK
        j_high = (HALO + first + TQ - 1) // TK + 1

        def scores(j, top):
            at = pl.multiple_of(j * TK, TK)
            k = kv_ref[pl.ds(at, TK), 0:128]
            s = lax.dot_general(
                both, k, (((1,), (1,)), ((), ())), preferred_element_type=jnp.float32
            )
            key = key_lane + at
            seen = (key >= start) & (key <= key_row + (HALO + first))
            seen = jnp.concatenate((seen, seen), axis=0)
            s = jnp.where(seen, s, -1e30)
            s_ref[j - j_low] = s
            return jnp.maximum(top, jnp.maximum(s[:, 0:128], s[:, 128:256]))

        top = lax.fori_loop(j_low, j_high, scores, jnp.full((2 * TQ, 128), -1e30, jnp.float32))
        top = jnp.max(top, axis=1, keepdims=True)

        def gather(j, state):
            total, acc = state
            at = pl.multiple_of(j * TK, TK)
            v = kv_ref[pl.ds(at, TK), 128:256]
            w = jnp.exp2((s_ref[j - j_low] - top) * (SCALE * LOG2E))
            total = total + (w[:, 0:128] + w[:, 128:256])
            acc = acc + jnp.dot(w.astype(jnp.bfloat16), v, preferred_element_type=jnp.float32)
            return total, acc

        zero = jnp.zeros((2 * TQ, 128), jnp.float32)
        total, acc = lax.fori_loop(j_low, j_high, gather, (zero, zero))
        total = jnp.sum(total, axis=1, keepdims=True)
        result = (acc / total).astype(jnp.bfloat16)
        out_ref[pl.ds(first, TQ), 0:128] = result[0:TQ]
        out_ref[pl.ds(first, TQ), 128:256] = result[TQ : 2 * TQ]
        norm = top * SCALE + jnp.log(total)
        slot = (i // 2) * 4 + i % 2
        held = norm_acc[...]
        held = jnp.where(lanes == slot, norm[0:TQ], held)
        held = jnp.where(lanes == slot + 2, norm[TQ : 2 * TQ], held)
        norm_acc[...] = held
        return carry

    lax.fori_loop(0, SPAN // TQ, block, 0)
    norm_ref[...] = jnp.transpose(norm_acc[...])[0:32]


def attend(low, start, qkv, halo):
    return pl.pallas_call(
        attend_body,
        in_specs=[
            pl.BlockSpec(memory_space=pltpu.SMEM),
            pl.BlockSpec(memory_space=pltpu.VMEM),
            pl.BlockSpec(memory_space=pltpu.VMEM),
            pl.BlockSpec(memory_space=pltpu.VMEM),
        ],
        out_specs=[
            pl.BlockSpec(memory_space=pltpu.VMEM),
            pl.BlockSpec(memory_space=pltpu.VMEM),
        ],
        out_shape=[
            jax.ShapeDtypeStruct((SPAN, 256), jnp.bfloat16),
            jax.ShapeDtypeStruct((32, 128), jnp.float32),
        ],
        scratch_shapes=[
            pltpu.VMEM((HALO + SPAN, 256), jnp.bfloat16),
            pltpu.VMEM((MOST_BLOCKS, 2 * TQ, TK), jnp.float32),
            pltpu.VMEM((TQ, 128), jnp.float32),
        ],
        name="attend",
    )(low, start, qkv, halo)


def per_device(queries, keys, values, lengths):
    row = lax.axis_index("z")
    base = lax.axis_index("x") * SPAN
    ends = jnp.cumsum(lax.dynamic_index_in_dim(lengths, row, 0, keepdims=False))
    pos = base + jnp.arange(SPAN, dtype=jnp.int32)
    doc_start = jnp.max(jnp.where(ends[None, :] <= pos[:, None], ends[None, :], 0), axis=1)
    start = doc_start - base + HALO
    low = start[:: TQ]
    start = jnp.broadcast_to(start[:, None], (SPAN, 128))

    packed = pack(queries, keys, values)
    moved = lax.all_to_all(packed, PLANE, 0, 0, tiled=True)
    qkv = moved.reshape(SPAN, 512)
    halo = lax.ppermute(qkv[SPAN - HALO :, 256:512], "x", [(i, i + 1) for i in range(3)])
    out, norm = attend(low, start, qkv, halo)
    back = lax.all_to_all(out.reshape(128, 16, 256), PLANE, 0, 0, tiled=True)
    attended = unpack(back)
    norm = lax.all_to_all(norm.reshape(8, 2, 256), "z", 0, 0, tiled=True)
    return attended, jnp.transpose(norm, (1, 0, 2))


def solution(mesh):
    split = Mesh(mesh.devices.reshape(4, 8, 8, 2), ALL)
    wide = P(None, ALL, None)
    return jax.shard_map(
        per_device,
        mesh=split,
        in_specs=(wide, wide, wide, P()),
        out_specs=(wide, P(("y", "c"), None, ("x", "z"))),
        check_vma=False,
    )
```

```python
import jax
import jax.numpy as jnp
from jax import lax
from jax.experimental import pallas as pl
from jax.experimental.pallas import tpu as pltpu
from jax.sharding import Mesh
from jax.sharding import PartitionSpec as P

HEAD = 128
ROWS = 8
KV_HEADS = 16
HALO = 1024
SPAN = 2048
TQ = 128
TK = 256
MOST_BLOCKS = 5
BLOCKS = SPAN // TQ
HALO_BLOCKS = HALO // TQ
LOG2E = 1.4426950408889634
SCALE = HEAD ** (-0.5)
ALL = ("x", "z", "y", "c")
PLANE = ("z", "y", "c")


def pack_body(q_ref, k_ref, v_ref, out_ref, sems):
    copies = []
    for h in range(KV_HEADS):
        for n, (ref, width, at) in enumerate(((q_ref, 256, 0), (k_ref, 128, 256), (v_ref, 128, 384))):
            copies.append(
                pltpu.make_async_copy(
                    ref.at[:, :, pl.ds(h * width, width)],
                    out_ref.at[:, h, :, pl.ds(at, width)],
                    sems.at[n, h],
                )
            )
    for copy in copies:
        copy.start()
    for copy in copies:
        copy.wait()


def pack(queries, keys, values):
    return pl.pallas_call(
        pack_body,
        in_specs=[pl.BlockSpec(memory_space=pl.ANY)] * 3,
        out_specs=pl.BlockSpec(memory_space=pl.ANY),
        out_shape=jax.ShapeDtypeStruct((ROWS, KV_HEADS, 16, 512), jnp.bfloat16),
        scratch_shapes=[pltpu.SemaphoreType.DMA((3, KV_HEADS))],
        name="pack",
    )(queries, keys, values)


def unpack_body(in_ref, out_ref, sems):
    copies = [
        pltpu.make_async_copy(
            in_ref.at[:, h], out_ref.at[:, :, pl.ds(h * 256, 256)], sems.at[h]
        )
        for h in range(KV_HEADS)
    ]
    for copy in copies:
        copy.start()
    for copy in copies:
        copy.wait()


def unpack(parts):
    return pl.pallas_call(
        unpack_body,
        in_specs=[pl.BlockSpec(memory_space=pl.ANY)],
        out_specs=pl.BlockSpec(memory_space=pl.ANY),
        out_shape=jax.ShapeDtypeStruct((ROWS, 16, 4096), jnp.bfloat16),
        scratch_shapes=[pltpu.SemaphoreType.DMA((KV_HEADS,))],
        name="unpack",
    )(parts)


def attend_block(i, j_low, ends_ref, qkv_ref, kv_ref, out_ref, s_ref, norm_acc):
    first = pl.multiple_of(i * TQ, TQ)
    slot = (i // 2) * 4 + i % 2
    count = (HALO + first) // TK + 1 - j_low

    def body(blocks):
        q = qkv_ref[pl.ds(first, TQ), 0:256]
        both = jnp.concatenate((q[:, 0:128], q[:, 128:256]), axis=0)
        row = lax.broadcasted_iota(jnp.int32, (TQ, TK), 0) + (HALO + first)
        top = None
        for n in range(blocks):
            at = pl.multiple_of((j_low + n) * TK, TK)
            s = lax.dot_general(
                both,
                kv_ref[pl.ds(at, TK), 0:128],
                (((1,), (1,)), ((), ())),
                preferred_element_type=jnp.float32,
            )
            seen = row < ends_ref[pl.ds(j_low + n, 1), :]
            if n == blocks - 1:
                seen = seen & (lax.broadcasted_iota(jnp.int32, (TQ, TK), 1) + at <= row)
            halves = []
            for h in range(2):
                part = jnp.where(seen, s[h * TQ : (h + 1) * TQ], -1e30)
                s_ref[n, h * TQ : (h + 1) * TQ] = part
                halves.append(jnp.maximum(part[:, 0:128], part[:, 128:256]))
            here = jnp.concatenate(halves, axis=0)
            top = here if top is None else jnp.maximum(top, here)
        top = jnp.max(top, axis=1, keepdims=True)
        total = acc = None
        for n in range(blocks):
            at = pl.multiple_of((j_low + n) * TK, TK)
            w = jnp.exp2((s_ref[n] - top) * (SCALE * LOG2E))
            part = w[:, 0:128] + w[:, 128:256]
            o = jnp.dot(
                w.astype(jnp.bfloat16),
                kv_ref[pl.ds(at, TK), 128:256],
                preferred_element_type=jnp.float32,
            )
            total = part if total is None else total + part
            acc = o if acc is None else acc + o
        total = jnp.sum(total, axis=1, keepdims=True)
        result = (acc / total).astype(jnp.bfloat16)
        out_ref[pl.ds(first, TQ), 0:128] = result[0:TQ]
        out_ref[pl.ds(first, TQ), 128:256] = result[TQ : 2 * TQ]
        norm = top * SCALE + jnp.log(total)
        lanes = lax.broadcasted_iota(jnp.int32, (TQ, 128), 1)
        held = jnp.where(lanes == slot, norm[0:TQ], norm_acc[...])
        norm_acc[...] = jnp.where(lanes == slot + 2, norm[TQ : 2 * TQ], held)

    for blocks in range(1, MOST_BLOCKS + 1):

        @pl.when(count == blocks)
        def _():
            body(blocks)


def local_body(low_ref, ends_ref, qkv_ref, out_ref, norm_ref, kv_ref, s_ref):
    kv_ref[HALO : HALO + SPAN] = qkv_ref[:, 256:512]
    norm_ref[...] = jnp.zeros((TQ, 128), jnp.float32)

    def block(i, carry):
        @pl.when(low_ref[i] >= HALO)
        def _():
            attend_block(i, low_ref[i] // TK, ends_ref, qkv_ref, kv_ref, out_ref, s_ref, norm_ref)

        return carry

    lax.fori_loop(0, BLOCKS, block, 0)


def attend_local(low, ends, qkv):
    vmem = pl.BlockSpec(memory_space=pltpu.VMEM)
    return pl.pallas_call(
        local_body,
        in_specs=[pl.BlockSpec(memory_space=pltpu.SMEM), vmem, vmem],
        out_specs=[vmem, vmem],
        out_shape=[
            jax.ShapeDtypeStruct((SPAN, 256), jnp.bfloat16),
            jax.ShapeDtypeStruct((TQ, 128), jnp.float32),
        ],
        scratch_shapes=[
            pltpu.VMEM((HALO + SPAN, 256), jnp.bfloat16),
            pltpu.VMEM((MOST_BLOCKS, 2 * TQ, TK), jnp.float32),
        ],
        name="attend_local",
    )(low, ends, qkv)


def halo_body(low_ref, ends_ref, qkv_ref, halo_ref, prev_ref, prev_norm, out_ref, norm_ref, kv_ref, s_ref, norm_acc):
    kv_ref[0:HALO] = halo_ref[...]
    kv_ref[HALO : 2 * HALO] = qkv_ref[:, 256:512]
    out_ref[...] = prev_ref[...]
    norm_acc[...] = prev_norm[...]

    def block(i, carry):
        @pl.when(low_ref[i] < HALO)
        def _():
            attend_block(i, low_ref[i] // TK, ends_ref, qkv_ref, kv_ref, out_ref, s_ref, norm_acc)

        return carry

    lax.fori_loop(0, HALO_BLOCKS, block, 0)
    norm_ref[...] = jnp.transpose(norm_acc[...])[0:32]


def attend_halo(low, ends, qkv, halo, out, norm):
    at_first = lambda *shape: pl.BlockSpec(shape, lambda n: (0, 0))
    return pl.pallas_call(
        halo_body,
        grid=(1,),
        in_specs=[
            pl.BlockSpec(memory_space=pltpu.SMEM),
            at_first(12, TK),
            at_first(HALO, 512),
            at_first(HALO, 256),
            at_first(HALO, 256),
            at_first(TQ, 128),
        ],
        out_specs=[at_first(HALO, 256), at_first(32, 128)],
        out_shape=[
            jax.ShapeDtypeStruct((SPAN, 256), jnp.bfloat16),
            jax.ShapeDtypeStruct((32, 128), jnp.float32),
        ],
        scratch_shapes=[
            pltpu.VMEM((2 * HALO, 256), jnp.bfloat16),
            pltpu.VMEM((MOST_BLOCKS, 2 * TQ, TK), jnp.float32),
            pltpu.VMEM((TQ, 128), jnp.float32),
        ],
        input_output_aliases={4: 0},
        name="attend_halo",
    )(low, ends, qkv, halo, out, norm)


def doc_bounds(lengths, row, base):
    own = lax.dynamic_index_in_dim(lengths, row, 0, keepdims=False)
    upto = jnp.arange(32)[:, None] <= jnp.arange(32)[None, :]
    ends = jnp.sum(jnp.where(upto, own[:, None], 0), axis=0)
    first = base + jnp.arange(BLOCKS, dtype=jnp.int32) * TQ
    low = jnp.max(jnp.where(ends[None, :] <= first[:, None], ends[None, :], 0), axis=1)
    pos = (base - HALO) + jnp.arange(HALO + SPAN, dtype=jnp.int32).reshape(12, TK)
    after = jnp.where(ends[:, None, None] > pos[None], ends[:, None, None], 1 << 20)
    end = jnp.where(pos >= 0, jnp.min(after, axis=0), -(1 << 20))
    return low - base + HALO, end - base + HALO


def per_device(queries, keys, values, lengths):
    low, ends = doc_bounds(lengths, lax.axis_index("z"), lax.axis_index("x") * SPAN)
    packed = pack(queries, keys, values).reshape(128, 16, 512)
    moved = lax.all_to_all(packed, PLANE, 0, 0, tiled=True)
    qkv = moved.reshape(SPAN, 512)
    halo = lax.ppermute(qkv[SPAN - HALO :, 256:512], "x", [(i, i + 1) for i in range(3)])
    out, norm = attend_local(low, ends, qkv)
    out, norm = attend_halo(low, ends, qkv, halo, out, norm)
    back = lax.all_to_all(out.reshape(128, 16, 256), PLANE, 0, 0, tiled=True)
    attended = unpack(back.reshape(ROWS, KV_HEADS, 16, 256))
    norms = lax.all_gather(norm, "z", axis=0, tiled=False)
    norms = lax.dynamic_slice_in_dim(norms, lax.axis_index("z") * 4, 4, 1)
    return attended, jnp.transpose(norms.reshape(8, 2, 256), (1, 0, 2))


def solution(mesh):
    split = Mesh(mesh.devices.reshape(4, 8, 8, 2), ALL)
    wide = P(None, ALL, None)
    return jax.shard_map(
        per_device,
        mesh=split,
        in_specs=(wide, wide, wide, P()),
        out_specs=(wide, P(("y", "c"), None, ("x", "z"))),
        check_vma=False,
    )
```

```python
import jax
import jax.numpy as jnp
from jax import lax
from jax.experimental import pallas as pl
from jax.experimental.pallas import tpu as pltpu
from jax.sharding import Mesh
from jax.sharding import PartitionSpec as P

HEAD = 128
ROWS = 8
KV_HEADS = 16
HALO = 1024
SPAN = 2048
TQ = 128
TK = 256
MOST_BLOCKS = 5
BLOCKS = SPAN // TQ
HALO_BLOCKS = HALO // TQ
LOG2E = 1.4426950408889634
SCALE = HEAD ** (-0.5)
ALL = ("x", "z", "y", "c")
PLANE = ("z", "y", "c")


def in_vmem(*arrays):
    return [pltpu.with_memory_space_constraint(a, pltpu.VMEM) for a in arrays]


def pack_body(q_ref, k_ref, v_ref, out_ref, held_ref, sems):
    parts = ((q_ref, 256, 0), (k_ref, 128, 256), (v_ref, 128, 384))
    reads = [
        [
            pltpu.make_async_copy(
                ref.at[:, :, pl.ds(h * width, width)],
                held_ref.at[:, h, :, pl.ds(at, width)],
                sems.at[n, h],
            )
            for n, (ref, width, at) in enumerate(parts)
        ]
        for h in range(KV_HEADS)
    ]
    writes = [
        pltpu.make_async_copy(held_ref.at[:, h], out_ref.at[:, h], sems.at[3, h])
        for h in range(KV_HEADS)
    ]
    for copies in reads:
        for copy in copies:
            copy.start()
    for h in range(KV_HEADS):
        for copy in reads[h]:
            copy.wait()
        writes[h].start()
    for copy in writes:
        copy.wait()


def pack(queries, keys, values):
    return pl.pallas_call(
        pack_body,
        in_specs=[pl.BlockSpec(memory_space=pl.ANY)] * 3,
        out_specs=pl.BlockSpec(memory_space=pl.ANY),
        out_shape=jax.ShapeDtypeStruct((ROWS, KV_HEADS, 16, 512), jnp.bfloat16),
        scratch_shapes=[
            pltpu.VMEM((ROWS, KV_HEADS, 16, 512), jnp.bfloat16),
            pltpu.SemaphoreType.DMA((4, KV_HEADS)),
        ],
        name="pack",
    )(queries, keys, values)


def unpack_body(in_ref, out_ref, sems):
    copies = [
        pltpu.make_async_copy(
            in_ref.at[:, h], out_ref.at[:, :, pl.ds(h * 256, 256)], sems.at[h]
        )
        for h in range(KV_HEADS)
    ]
    for copy in copies:
        copy.start()
    for copy in copies:
        copy.wait()


def unpack(parts):
    return pl.pallas_call(
        unpack_body,
        in_specs=[pl.BlockSpec(memory_space=pltpu.VMEM)],
        out_specs=pl.BlockSpec(memory_space=pl.ANY),
        out_shape=jax.ShapeDtypeStruct((ROWS, 16, 4096), jnp.bfloat16),
        scratch_shapes=[pltpu.SemaphoreType.DMA((KV_HEADS,))],
        name="unpack",
    )(*in_vmem(parts))


def attend_block(i, j_low, ends_ref, qkv_ref, keys_at, values_at, out_ref, s_ref, norm_acc):
    first = pl.multiple_of(i * TQ, TQ)
    slot = (i // 2) * 4 + i % 2
    count = (HALO + first) // TK + 1 - j_low

    def body(blocks):
        q = qkv_ref[pl.ds(first, TQ), 0:256]
        both = jnp.concatenate((q[:, 0:128], q[:, 128:256]), axis=0)
        row = lax.broadcasted_iota(jnp.int32, (TQ, TK), 0) + (HALO + first)
        top = None
        for n in range(blocks):
            at = pl.multiple_of((j_low + n) * TK, TK)
            s = lax.dot_general(
                both,
                keys_at(at),
                (((1,), (1,)), ((), ())),
                preferred_element_type=jnp.float32,
            )
            seen = row < ends_ref[pl.ds(j_low + n, 1), :]
            if n == blocks - 1:
                seen = seen & (lax.broadcasted_iota(jnp.int32, (TQ, TK), 1) + at <= row)
            halves = []
            for h in range(2):
                part = jnp.where(seen, s[h * TQ : (h + 1) * TQ], -1e30)
                s_ref[n, h * TQ : (h + 1) * TQ] = part
                halves.append(jnp.maximum(part[:, 0:128], part[:, 128:256]))
            here = jnp.concatenate(halves, axis=0)
            top = here if top is None else jnp.maximum(top, here)
        top = jnp.max(top, axis=1, keepdims=True)
        total = acc = None
        for n in range(blocks):
            at = pl.multiple_of((j_low + n) * TK, TK)
            w = jnp.exp2((s_ref[n] - top) * (SCALE * LOG2E))
            part = w[:, 0:128] + w[:, 128:256]
            o = jnp.dot(
                w.astype(jnp.bfloat16),
                values_at(at),
                preferred_element_type=jnp.float32,
            )
            total = part if total is None else total + part
            acc = o if acc is None else acc + o
        total = jnp.sum(total, axis=1, keepdims=True)
        result = (acc / total).astype(jnp.bfloat16)
        out_ref[i, :, 0:128] = result[0:TQ]
        out_ref[i, :, 128:256] = result[TQ : 2 * TQ]
        norm = top * SCALE + jnp.log(total)
        lanes = lax.broadcasted_iota(jnp.int32, (TQ, 128), 1)
        held = jnp.where(lanes == slot, norm[0:TQ], norm_acc[...])
        norm_acc[...] = jnp.where(lanes == slot + 2, norm[TQ : 2 * TQ], held)

    for blocks in range(1, MOST_BLOCKS + 1):

        @pl.when(count == blocks)
        def _():
            body(blocks)


def out_copy(i, held_ref, out_ref, sems):
    return pltpu.make_async_copy(held_ref.at[i], out_ref.at[pl.ds(i * TQ, TQ)], sems.at[i])


def local_body(low_ref, ends_ref, qkv_ref, out_ref, norm_ref, held_ref, s_ref, sems):
    norm_ref[...] = jnp.zeros((TQ, 128), jnp.float32)
    keys_at = lambda at: qkv_ref[pl.ds(pl.multiple_of(at - HALO, TK), TK), 256:384]
    values_at = lambda at: qkv_ref[pl.ds(pl.multiple_of(at - HALO, TK), TK), 384:512]

    def block(i, carry):
        @pl.when(low_ref[i] >= HALO)
        def _():
            attend_block(
                i, low_ref[i] // TK, ends_ref, qkv_ref, keys_at, values_at, held_ref, s_ref, norm_ref
            )
            out_copy(i, held_ref, out_ref, sems).start()

        return carry

    lax.fori_loop(0, BLOCKS, block, 0)
    for i in range(BLOCKS):

        @pl.when(low_ref[i] >= HALO)
        def _():
            out_copy(i, held_ref, out_ref, sems).wait()


def attend_local(low, ends, qkv):
    vmem = pl.BlockSpec(memory_space=pltpu.VMEM)
    return pl.pallas_call(
        local_body,
        in_specs=[pl.BlockSpec(memory_space=pltpu.SMEM), vmem, vmem],
        out_specs=[pl.BlockSpec(memory_space=pl.ANY), vmem],
        out_shape=[
            jax.ShapeDtypeStruct((SPAN, 256), jnp.bfloat16),
            jax.ShapeDtypeStruct((TQ, 128), jnp.float32),
        ],
        scratch_shapes=[
            pltpu.VMEM((BLOCKS, TQ, 256), jnp.bfloat16),
            pltpu.VMEM((MOST_BLOCKS, 2 * TQ, TK), jnp.float32),
            pltpu.SemaphoreType.DMA((BLOCKS,)),
        ],
        name="attend_local",
    )(low, ends, *in_vmem(qkv))


def halo_body(
    low_ref, ends_ref, qkv_ref, halo_ref, prev_ref, prev_norm, out_ref, norm_ref, kv_ref, held_ref, s_ref, norm_acc, sems
):
    kv_ref[0:HALO] = halo_ref[...]
    kv_ref[HALO : 2 * HALO] = qkv_ref[0:HALO, 256:512]
    norm_acc[...] = prev_norm[...]
    keys_at = lambda at: kv_ref[pl.ds(at, TK), 0:128]
    values_at = lambda at: kv_ref[pl.ds(at, TK), 128:256]

    def block(i, carry):
        @pl.when(low_ref[i] < HALO)
        def _():
            attend_block(
                i, low_ref[i] // TK, ends_ref, qkv_ref, keys_at, values_at, held_ref, s_ref, norm_acc
            )
            out_copy(i, held_ref, out_ref, sems).start()

        return carry

    lax.fori_loop(0, HALO_BLOCKS, block, 0)
    norm_ref[...] = jnp.transpose(norm_acc[...])[0:32]
    for i in range(HALO_BLOCKS):

        @pl.when(low_ref[i] < HALO)
        def _():
            out_copy(i, held_ref, out_ref, sems).wait()


def attend_halo(low, ends, qkv, halo, out, norm):
    vmem = pl.BlockSpec(memory_space=pltpu.VMEM)
    return pl.pallas_call(
        halo_body,
        in_specs=[
            pl.BlockSpec(memory_space=pltpu.SMEM),
            vmem,
            vmem,
            vmem,
            pl.BlockSpec(memory_space=pl.ANY),
            vmem,
        ],
        out_specs=[pl.BlockSpec(memory_space=pl.ANY), vmem],
        out_shape=[
            jax.ShapeDtypeStruct((SPAN, 256), jnp.bfloat16),
            pltpu.VMEM((32, 128), jnp.float32),
        ],
        scratch_shapes=[
            pltpu.VMEM((2 * HALO, 256), jnp.bfloat16),
            pltpu.VMEM((HALO_BLOCKS, TQ, 256), jnp.bfloat16),
            pltpu.VMEM((MOST_BLOCKS, 2 * TQ, TK), jnp.float32),
            pltpu.VMEM((TQ, 128), jnp.float32),
            pltpu.SemaphoreType.DMA((HALO_BLOCKS,)),
        ],
        input_output_aliases={4: 0},
        name="attend_halo",
    )(low, ends, *in_vmem(qkv, halo), out, norm)


def doc_bounds(lengths, row, base):
    own = lax.dynamic_index_in_dim(lengths, row, 0, keepdims=False)
    upto = jnp.arange(32)[:, None] <= jnp.arange(32)[None, :]
    ends = jnp.sum(jnp.where(upto, own[:, None], 0), axis=0)
    first = base + jnp.arange(BLOCKS, dtype=jnp.int32) * TQ
    low = jnp.max(jnp.where(ends[None, :] <= first[:, None], ends[None, :], 0), axis=1)
    pos = (base - HALO) + jnp.arange(HALO + SPAN, dtype=jnp.int32).reshape(12, TK)
    after = jnp.where(ends[:, None, None] > pos[None], ends[:, None, None], 1 << 20)
    end = jnp.where(pos >= 0, jnp.min(after, axis=0), -(1 << 20))
    return low - base + HALO, end - base + HALO


def per_device(queries, keys, values, lengths):
    low, ends = doc_bounds(lengths, lax.axis_index("z"), lax.axis_index("x") * SPAN)
    packed = pack(queries, keys, values).reshape(128, 16, 512)
    moved = lax.all_to_all(packed, PLANE, 0, 0, tiled=True)
    qkv = moved.reshape(SPAN, 512)
    halo = lax.ppermute(qkv[SPAN - HALO :, 256:512], "x", [(i, i + 1) for i in range(3)])
    out, norm = attend_local(low, ends, qkv)
    out, norm = attend_halo(low, ends, qkv, halo, out, norm)
    back = lax.all_to_all(out.reshape(128, 16, 256), PLANE, 0, 0, tiled=True)
    attended = unpack(back.reshape(ROWS, KV_HEADS, 16, 256))
    norms = lax.all_gather(norm, "z", axis=0, tiled=False)
    norms = lax.dynamic_slice_in_dim(norms, lax.axis_index("z") * 4, 4, 1)
    return attended, jnp.transpose(norms.reshape(8, 2, 256), (1, 0, 2))


def solution(mesh):
    split = Mesh(mesh.devices.reshape(4, 8, 8, 2), ALL)
    wide = P(None, ALL, None)
    return jax.shard_map(
        per_device,
        mesh=split,
        in_specs=(wide, wide, wide, P()),
        out_specs=(wide, P(("y", "c"), None, ("x", "z"))),
        check_vma=False,
    )
```

```python
import jax
import jax.numpy as jnp
from jax import lax
from jax.experimental import pallas as pl
from jax.experimental.pallas import tpu as pltpu
from jax.sharding import Mesh
from jax.sharding import PartitionSpec as P

HEAD = 128
ROWS = 8
KV_HEADS = 16
HALO = 1024
SPAN = 2048
TQ = 128
TK = 256
MOST_BLOCKS = 5
BLOCKS = SPAN // TQ
HALO_BLOCKS = HALO // TQ
FAR = 1 << 20
LOG2E = 1.4426950408889634
SCALE = HEAD ** (-0.5)
ALL = ("x", "z", "y", "c")
PLANE = ("z", "y", "c")


def in_vmem(*arrays):
    return [pltpu.with_memory_space_constraint(a, pltpu.VMEM) for a in arrays]


def doc_bounds(lengths_ref, row, base, low_ref, ends_ref):
    origin = HALO - base
    slot = lax.broadcasted_iota(jnp.int32, (12, TK), 0) * TK
    slot = slot + lax.broadcasted_iota(jnp.int32, (12, TK), 1)
    end = origin
    low = [origin] * BLOCKS
    after = jnp.full((12, TK), FAR, jnp.int32)
    for n in range(32):
        end = end + lengths_ref[row, n]
        low = [jnp.where(end <= HALO + i * TQ, end, low[i]) for i in range(BLOCKS)]
        after = jnp.minimum(after, jnp.where(slot < end, end, FAR))
    ends_ref[...] = jnp.where(slot < origin, 0, after)
    for i in range(BLOCKS):
        low_ref[i] = low[i]
    low_ref[BLOCKS] = row


def bounds_body(lengths_ref, row_ref, base_ref, low_ref, ends_ref):
    doc_bounds(lengths_ref, row_ref[0], base_ref[0], low_ref, ends_ref)


def bounds(lengths, row, base):
    smem = pl.BlockSpec(memory_space=pltpu.SMEM)
    return pl.pallas_call(
        bounds_body,
        in_specs=[smem] * 3,
        out_specs=[smem, pl.BlockSpec(memory_space=pltpu.VMEM)],
        out_shape=[
            jax.ShapeDtypeStruct((BLOCKS + 1,), jnp.int32),
            jax.ShapeDtypeStruct((12, TK), jnp.int32),
        ],
        name="doc_bounds",
    )(lengths, row, base)


def pack_body(q_ref, k_ref, v_ref, out_ref, held_ref, sems):
    parts = ((q_ref, 256, 0), (k_ref, 128, 256), (v_ref, 128, 384))
    reads = [
        [
            pltpu.make_async_copy(
                ref.at[:, :, pl.ds(h * width, width)],
                held_ref.at[:, h, :, pl.ds(at, width)],
                sems.at[n, h],
            )
            for n, (ref, width, at) in enumerate(parts)
        ]
        for h in range(KV_HEADS)
    ]
    writes = [
        pltpu.make_async_copy(held_ref.at[:, h], out_ref.at[:, h], sems.at[3, h])
        for h in range(KV_HEADS)
    ]
    for copies in reads:
        for copy in copies:
            copy.start()
    for h in range(KV_HEADS):
        for copy in reads[h]:
            copy.wait()
        writes[h].start()
    for copy in writes:
        copy.wait()


def pack(queries, keys, values):
    return pl.pallas_call(
        pack_body,
        in_specs=[pl.BlockSpec(memory_space=pl.ANY)] * 3,
        out_specs=pl.BlockSpec(memory_space=pl.ANY),
        out_shape=jax.ShapeDtypeStruct((ROWS, KV_HEADS, 16, 512), jnp.bfloat16),
        scratch_shapes=[
            pltpu.VMEM((ROWS, KV_HEADS, 16, 512), jnp.bfloat16),
            pltpu.SemaphoreType.DMA((4, KV_HEADS)),
        ],
        name="pack",
    )(queries, keys, values)


def unpack_body(in_ref, out_ref, sems):
    copies = [
        pltpu.make_async_copy(
            in_ref.at[:, h], out_ref.at[:, :, pl.ds(h * 256, 256)], sems.at[h]
        )
        for h in range(KV_HEADS)
    ]
    for copy in copies:
        copy.start()
    for copy in copies:
        copy.wait()


def unpack(parts):
    return pl.pallas_call(
        unpack_body,
        in_specs=[pl.BlockSpec(memory_space=pltpu.VMEM)],
        out_specs=pl.BlockSpec(memory_space=pl.ANY),
        out_shape=jax.ShapeDtypeStruct((ROWS, 16, 4096), jnp.bfloat16),
        scratch_shapes=[pltpu.SemaphoreType.DMA((KV_HEADS,))],
        name="unpack",
    )(*in_vmem(parts))


def attend_block(i, j_low, ends_ref, qkv_ref, keys_at, values_at, out_ref, s_ref, norm_acc):
    first = pl.multiple_of(i * TQ, TQ)
    slot = (i // 2) * 8 + i % 2
    count = (HALO + first) // TK + 1 - j_low

    def body(blocks):
        q = qkv_ref[pl.ds(first, TQ), 0:256]
        both = jnp.concatenate((q[:, 0:128], q[:, 128:256]), axis=0)
        row = lax.broadcasted_iota(jnp.int32, (TQ, TK), 0) + (HALO + first)
        top = None
        for n in range(blocks):
            at = pl.multiple_of((j_low + n) * TK, TK)
            s = lax.dot_general(
                both,
                keys_at(at),
                (((1,), (1,)), ((), ())),
                preferred_element_type=jnp.float32,
            )
            seen = row < ends_ref[pl.ds(j_low + n, 1), :]
            if n == blocks - 1:
                seen = seen & (lax.broadcasted_iota(jnp.int32, (TQ, TK), 1) + at <= row)
            halves = []
            for h in range(2):
                part = jnp.where(seen, s[h * TQ : (h + 1) * TQ], -1e30)
                s_ref[n, h * TQ : (h + 1) * TQ] = part
                halves.append(jnp.maximum(part[:, 0:128], part[:, 128:256]))
            here = jnp.concatenate(halves, axis=0)
            top = here if top is None else jnp.maximum(top, here)
        top = jnp.max(top, axis=1, keepdims=True)
        total = acc = None
        for n in range(blocks):
            at = pl.multiple_of((j_low + n) * TK, TK)
            w = jnp.exp2((s_ref[n] - top) * (SCALE * LOG2E))
            part = w[:, 0:128] + w[:, 128:256]
            o = jnp.dot(
                w.astype(jnp.bfloat16),
                values_at(at),
                preferred_element_type=jnp.float32,
            )
            total = part if total is None else total + part
            acc = o if acc is None else acc + o
        total = jnp.sum(total, axis=1, keepdims=True)
        result = (acc / total).astype(jnp.bfloat16)
        out_ref[i, :, 0:128] = result[0:TQ]
        out_ref[i, :, 128:256] = result[TQ : 2 * TQ]
        norm = top * SCALE + jnp.log(total)
        lanes = lax.broadcasted_iota(jnp.int32, (TQ, 128), 1)
        held = jnp.where(lanes == slot, norm[0:TQ], norm_acc[...])
        norm_acc[...] = jnp.where(lanes == slot + 2, norm[TQ : 2 * TQ], held)

    for blocks in range(1, MOST_BLOCKS + 1):

        @pl.when(count == blocks)
        def _():
            body(blocks)


def out_copy(i, held_ref, out_ref, sems):
    return pltpu.make_async_copy(held_ref.at[i], out_ref.at[pl.ds(i * TQ, TQ)], sems.at[i])


def local_body(low_ref, ends_ref, qkv_ref, out_ref, norm_ref, held_ref, s_ref, sems):
    norm_ref[...] = jnp.zeros((TQ, 128), jnp.float32)
    keys_at = lambda at: qkv_ref[pl.ds(pl.multiple_of(at - HALO, TK), TK), 256:384]
    values_at = lambda at: qkv_ref[pl.ds(pl.multiple_of(at - HALO, TK), TK), 384:512]

    def block(i, carry):
        @pl.when(low_ref[i] >= HALO)
        def _():
            attend_block(
                i, low_ref[i] // TK, ends_ref, qkv_ref, keys_at, values_at, held_ref, s_ref, norm_ref
            )
            out_copy(i, held_ref, out_ref, sems).start()

        return carry

    lax.fori_loop(0, BLOCKS, block, 0)
    for i in range(BLOCKS):

        @pl.when(low_ref[i] >= HALO)
        def _():
            out_copy(i, held_ref, out_ref, sems).wait()


def attend_local(low, ends, qkv):
    vmem = pl.BlockSpec(memory_space=pltpu.VMEM)
    return pl.pallas_call(
        local_body,
        in_specs=[pl.BlockSpec(memory_space=pltpu.SMEM), vmem, vmem],
        out_specs=[pl.BlockSpec(memory_space=pl.ANY), vmem],
        out_shape=[
            jax.ShapeDtypeStruct((SPAN, 256), jnp.bfloat16),
            jax.ShapeDtypeStruct((TQ, 128), jnp.float32),
        ],
        scratch_shapes=[
            pltpu.VMEM((BLOCKS, TQ, 256), jnp.bfloat16),
            pltpu.VMEM((MOST_BLOCKS, 2 * TQ, TK), jnp.float32),
            pltpu.SemaphoreType.DMA((BLOCKS,)),
        ],
        name="attend_local",
    )(low, ends, *in_vmem(qkv))


def halo_body(
    low_ref, ends_ref, qkv_ref, halo_ref, prev_ref, prev_norm, *refs
):
    out_ref, *norm_refs = refs[:9]
    kv_ref, held_ref, s_ref, norm_acc, norm_t, sems = refs[9:]
    kv_ref[0:HALO] = halo_ref[...]
    kv_ref[HALO : 2 * HALO] = qkv_ref[0:HALO, 256:512]
    norm_acc[...] = prev_norm[...]
    keys_at = lambda at: kv_ref[pl.ds(at, TK), 0:128]
    values_at = lambda at: kv_ref[pl.ds(at, TK), 128:256]

    def block(i, carry):
        @pl.when(low_ref[i] < HALO)
        def _():
            attend_block(
                i, low_ref[i] // TK, ends_ref, qkv_ref, keys_at, values_at, held_ref, s_ref, norm_acc
            )
            out_copy(i, held_ref, out_ref, sems).start()

        return carry

    lax.fori_loop(0, HALO_BLOCKS, block, 0)
    norm_t[...] = jnp.transpose(norm_acc[...])
    for d in range(8):
        norm_refs[d][...] = norm_t[pl.ds(pl.multiple_of(((low_ref[BLOCKS] + d) % 8) * 8, 8), 8)]
    for i in range(HALO_BLOCKS):

        @pl.when(low_ref[i] < HALO)
        def _():
            out_copy(i, held_ref, out_ref, sems).wait()


def attend_halo(low, ends, qkv, halo, out, norm):
    vmem = pl.BlockSpec(memory_space=pltpu.VMEM)
    return pl.pallas_call(
        halo_body,
        in_specs=[
            pl.BlockSpec(memory_space=pltpu.SMEM),
            vmem,
            vmem,
            vmem,
            pl.BlockSpec(memory_space=pl.ANY),
            vmem,
        ],
        out_specs=[pl.BlockSpec(memory_space=pl.ANY)] + [vmem] * 8,
        out_shape=[jax.ShapeDtypeStruct((SPAN, 256), jnp.bfloat16)]
        + [pltpu.VMEM((8, 128), jnp.float32)] * 8,
        scratch_shapes=[
            pltpu.VMEM((2 * HALO, 256), jnp.bfloat16),
            pltpu.VMEM((HALO_BLOCKS, TQ, 256), jnp.bfloat16),
            pltpu.VMEM((MOST_BLOCKS, 2 * TQ, TK), jnp.float32),
            pltpu.VMEM((TQ, 128), jnp.float32),
            pltpu.VMEM((TQ, 128), jnp.float32),
            pltpu.SemaphoreType.DMA((HALO_BLOCKS,)),
        ],
        input_output_aliases={4: 0},
        name="attend_halo",
    )(low, ends, *in_vmem(qkv, halo), out, norm)


def norm_body(row_ref, *refs):
    *pieces, out_ref = refs
    rows = lax.broadcasted_iota(jnp.int32, (8, 128), 0)
    for h in range(2):
        for n in range(2):
            at = 2 * h + n
            held = jnp.zeros((8, 128), jnp.float32)
            for d in range(8):
                held = jnp.where(rows == (row_ref[0] + 8 - d) % 8, pieces[d][at : at + 1], held)
            out_ref[h, :, n * 128 : (n + 1) * 128] = held


def norm_rows(row, pieces):
    vmem = pl.BlockSpec(memory_space=pltpu.VMEM)
    return pl.pallas_call(
        norm_body,
        in_specs=[pl.BlockSpec(memory_space=pltpu.SMEM)] + [vmem] * 8,
        out_specs=vmem,
        out_shape=jax.ShapeDtypeStruct((2, ROWS, 256), jnp.float32),
        name="norm_rows",
    )(row, *pieces)


def per_device(queries, keys, values, lengths):
    row = lax.axis_index("z")
    base = lax.axis_index("x") * SPAN
    packed = pack(queries, keys, values).reshape(128, 16, 512)
    moved = lax.all_to_all(packed, PLANE, 0, 0, tiled=True)
    low, ends = bounds(lengths, row[None], base[None])
    qkv = moved.reshape(SPAN, 512)
    halo = lax.ppermute(qkv[SPAN - HALO :, 256:512], "x", [(i, i + 1) for i in range(3)])
    out, norm = attend_local(low, ends, qkv)
    out, *norms = attend_halo(low, ends, qkv, halo, out, norm)
    back = lax.all_to_all(out.reshape(128, 16, 256), PLANE, 0, 0, tiled=True)
    attended = unpack(back.reshape(ROWS, KV_HEADS, 16, 256))
    for d in range(1, 8):
        norms[d] = lax.ppermute(norms[d], "z", [(i, (i + d) % 8) for i in range(8)])
    return attended, norm_rows(row[None], norms)


def solution(mesh):
    split = Mesh(mesh.devices.reshape(4, 8, 8, 2), ALL)
    wide = P(None, ALL, None)
    return jax.shard_map(
        per_device,
        mesh=split,
        in_specs=(wide, wide, wide, P()),
        out_specs=(wide, P(("y", "c"), None, ("x", "z"))),
        check_vma=False,
    )
```

```python
import jax
import jax.numpy as jnp
from jax import lax
from jax.experimental import pallas as pl
from jax.experimental.pallas import tpu as pltpu
from jax.sharding import Mesh
from jax.sharding import PartitionSpec as P

HEAD = 128
ROWS = 8
KV_HEADS = 16
HALO = 1024
SPAN = 2048
TQ = 128
TK = 256
MOST_BLOCKS = 5
BLOCKS = SPAN // TQ
HALO_BLOCKS = HALO // TQ
FAR = 1 << 20
LOG2E = 1.4426950408889634
SCALE = HEAD ** (-0.5)
ALL = ("x", "z", "y", "c")
PLANE = ("z", "y", "c")


def in_vmem(*arrays):
    return [pltpu.with_memory_space_constraint(a, pltpu.VMEM) for a in arrays]


def doc_bounds(lengths_ref, row, base, low_ref, ends_ref):
    origin = HALO - base
    slot = lax.broadcasted_iota(jnp.int32, (12, TK), 0) * TK
    slot = slot + lax.broadcasted_iota(jnp.int32, (12, TK), 1)
    end = origin
    low = [origin] * BLOCKS
    after = jnp.full((12, TK), FAR, jnp.int32)
    for n in range(32):
        end = end + lengths_ref[row, n]
        low = [jnp.where(end <= HALO + i * TQ, end, low[i]) for i in range(BLOCKS)]
        after = jnp.minimum(after, jnp.where(slot < end, end, FAR))
    ends_ref[...] = jnp.where(slot < origin, 0, after)
    for i in range(BLOCKS):
        low_ref[i] = low[i]
    low_ref[BLOCKS] = row


def bounds_body(lengths_ref, row_ref, base_ref, low_ref, ends_ref):
    doc_bounds(lengths_ref, row_ref[0], base_ref[0], low_ref, ends_ref)


def bounds(lengths, row, base):
    smem = pl.BlockSpec(memory_space=pltpu.SMEM)
    return pl.pallas_call(
        bounds_body,
        in_specs=[smem] * 3,
        out_specs=[smem, pl.BlockSpec(memory_space=pltpu.VMEM)],
        out_shape=[
            jax.ShapeDtypeStruct((BLOCKS + 1,), jnp.int32),
            jax.ShapeDtypeStruct((12, TK), jnp.int32),
        ],
        name="doc_bounds",
    )(lengths, row, base)


def pack_body(q_ref, k_ref, v_ref, out_ref, held_ref, sems):
    parts = ((q_ref, 256, 0), (k_ref, 128, 256), (v_ref, 128, 384))
    reads = [
        [
            pltpu.make_async_copy(
                ref.at[:, :, pl.ds(h * width, width)],
                held_ref.at[:, h, :, pl.ds(at, width)],
                sems.at[n, h],
            )
            for n, (ref, width, at) in enumerate(parts)
        ]
        for h in range(KV_HEADS)
    ]
    writes = [
        pltpu.make_async_copy(held_ref.at[:, h], out_ref.at[:, h], sems.at[3, h])
        for h in range(KV_HEADS)
    ]
    for copies in reads:
        for copy in copies:
            copy.start()
    for h in range(KV_HEADS):
        for copy in reads[h]:
            copy.wait()
        writes[h].start()
    for copy in writes:
        copy.wait()


def pack(queries, keys, values):
    return pl.pallas_call(
        pack_body,
        in_specs=[pl.BlockSpec(memory_space=pl.ANY)] * 3,
        out_specs=pl.BlockSpec(memory_space=pl.ANY),
        out_shape=jax.ShapeDtypeStruct((ROWS, KV_HEADS, 16, 512), jnp.bfloat16),
        scratch_shapes=[
            pltpu.VMEM((ROWS, KV_HEADS, 16, 512), jnp.bfloat16),
            pltpu.SemaphoreType.DMA((4, KV_HEADS)),
        ],
        name="pack",
    )(queries, keys, values)


def unpack_body(row_ref, in_ref, *refs):
    *pieces, out_ref, norm_ref, sems = refs
    copies = [
        pltpu.make_async_copy(
            in_ref.at[:, h], out_ref.at[:, :, pl.ds(h * 256, 256)], sems.at[h]
        )
        for h in range(KV_HEADS)
    ]
    for copy in copies:
        copy.start()
    rows = lax.broadcasted_iota(jnp.int32, (8, 128), 0)
    for h in range(2):
        for n in range(2):
            at = 2 * h + n
            held = jnp.zeros((8, 128), jnp.float32)
            for d in range(8):
                held = jnp.where(rows == (row_ref[0] + 8 - d) % 8, pieces[d][at : at + 1], held)
            norm_ref[h, :, n * 128 : (n + 1) * 128] = held
    for copy in copies:
        copy.wait()


def unpack(row, parts, pieces):
    vmem = pl.BlockSpec(memory_space=pltpu.VMEM)
    return pl.pallas_call(
        unpack_body,
        in_specs=[pl.BlockSpec(memory_space=pltpu.SMEM)] + [vmem] * 9,
        out_specs=[pl.BlockSpec(memory_space=pl.ANY), vmem],
        out_shape=[
            jax.ShapeDtypeStruct((ROWS, 16, 4096), jnp.bfloat16),
            jax.ShapeDtypeStruct((2, ROWS, 256), jnp.float32),
        ],
        scratch_shapes=[pltpu.SemaphoreType.DMA((KV_HEADS,))],
        name="unpack",
    )(row, *in_vmem(parts, *pieces))


def partial_softmax(q, row, j_low, blocks, diagonal, ends_ref, keys_at, values_at, s_ref):
    both = jnp.concatenate((q[:, 0:128], q[:, 128:256]), axis=0)
    top = None
    for n in range(blocks):
        s = lax.dot_general(
            both,
            keys_at(j_low + n),
            (((1,), (1,)), ((), ())),
            preferred_element_type=jnp.float32,
        )
        seen = row < ends_ref[pl.ds(j_low + n, 1), :]
        if diagonal and n == blocks - 1:
            key = lax.broadcasted_iota(jnp.int32, (TQ, TK), 1) + (j_low + n) * TK
            seen = seen & (key <= row)
        halves = []
        for h in range(2):
            part = jnp.where(seen, s[h * TQ : (h + 1) * TQ], -1e30)
            s_ref[n, h * TQ : (h + 1) * TQ] = part
            halves.append(jnp.maximum(part[:, 0:128], part[:, 128:256]))
        here = jnp.concatenate(halves, axis=0)
        top = here if top is None else jnp.maximum(top, here)
    top = jnp.max(top, axis=1, keepdims=True)
    total = acc = None
    for n in range(blocks):
        w = jnp.exp2((s_ref[n] - top) * (SCALE * LOG2E))
        part = w[:, 0:128] + w[:, 128:256]
        o = jnp.dot(
            w.astype(jnp.bfloat16), values_at(j_low + n), preferred_element_type=jnp.float32
        )
        total = part if total is None else total + part
        acc = o if acc is None else acc + o
    return top, jnp.sum(total, axis=1, keepdims=True), acc


def out_copy(i, held_ref, out_ref, sems):
    return pltpu.make_async_copy(held_ref.at[i], out_ref.at[pl.ds(i * TQ, TQ)], sems.at[0, i])


def part_copy(i, src_ref, dst_ref, sems):
    return pltpu.make_async_copy(src_ref.at[i], dst_ref.at[i], sems.at[1, i])


def keep(held_ref, i, result):
    result = result.astype(jnp.bfloat16)
    held_ref[i, :, 0:128] = result[0:TQ]
    held_ref[i, :, 128:256] = result[TQ : 2 * TQ]


def norm_slot(i):
    return (i // 2) * 8 + i % 2


def keep_norm(norm_acc, i, norm):
    lanes = lax.broadcasted_iota(jnp.int32, (TQ, 128), 1)
    held = jnp.where(lanes == norm_slot(i), norm[0:TQ], norm_acc[...])
    norm_acc[...] = jnp.where(lanes == norm_slot(i) + 2, norm[TQ : 2 * TQ], held)


def local_body(
    low_ref, ends_ref, qkv_ref, out_ref, norm_ref, part_ref, held_ref, kept_ref, s_ref, sems
):
    norm_ref[...] = jnp.zeros((TQ, 128), jnp.float32)
    rows = lambda j: pl.ds(pl.multiple_of(j * TK - HALO, TK), TK)
    keys_at = lambda j: qkv_ref[rows(j), 256:384]
    values_at = lambda j: qkv_ref[rows(j), 384:512]

    def block(i, carry):
        first = pl.multiple_of(i * TQ, TQ)
        j_low = jnp.maximum(low_ref[i], HALO) // TK
        count = (HALO + first) // TK + 1 - j_low
        row = lax.broadcasted_iota(jnp.int32, (TQ, TK), 0) + (HALO + first)
        for blocks in range(1, MOST_BLOCKS + 1):

            @pl.when(count == blocks)
            def _():
                q = qkv_ref[pl.ds(first, TQ), 0:256]
                top, total, acc = partial_softmax(
                    q, row, j_low, blocks, True, ends_ref, keys_at, values_at, s_ref
                )
                result = acc / total
                kept_ref[i] = result
                keep(held_ref, i, result)
                keep_norm(norm_ref, i, top * SCALE + jnp.log(total))

        @pl.when(low_ref[i] >= HALO)
        def _():
            out_copy(i, held_ref, out_ref, sems).start()

        @pl.when(low_ref[i] < HALO)
        def _():
            part_copy(i, kept_ref, part_ref, sems).start()

        return carry

    lax.fori_loop(0, BLOCKS, block, 0)
    for i in range(BLOCKS):

        @pl.when(low_ref[i] >= HALO)
        def _():
            out_copy(i, held_ref, out_ref, sems).wait()

        if i < HALO_BLOCKS:

            @pl.when(low_ref[i] < HALO)
            def _():
                part_copy(i, kept_ref, part_ref, sems).wait()


def attend_local(low, ends, qkv):
    vmem = pl.BlockSpec(memory_space=pltpu.VMEM)
    any_space = pl.BlockSpec(memory_space=pl.ANY)
    return pl.pallas_call(
        local_body,
        in_specs=[pl.BlockSpec(memory_space=pltpu.SMEM), vmem, vmem],
        out_specs=[any_space, vmem, any_space],
        out_shape=[
            jax.ShapeDtypeStruct((SPAN, 256), jnp.bfloat16),
            jax.ShapeDtypeStruct((TQ, 128), jnp.float32),
            jax.ShapeDtypeStruct((HALO_BLOCKS, 2 * TQ, 128), jnp.float32),
        ],
        scratch_shapes=[
            pltpu.VMEM((BLOCKS, TQ, 256), jnp.bfloat16),
            pltpu.VMEM((BLOCKS, 2 * TQ, 128), jnp.float32),
            pltpu.VMEM((MOST_BLOCKS, 2 * TQ, TK), jnp.float32),
            pltpu.SemaphoreType.DMA((2, BLOCKS)),
        ],
        name="attend_local",
    )(low, ends, *in_vmem(qkv))


def halo_body(low_ref, ends_ref, qkv_ref, halo_ref, prev_ref, prev_norm, part_ref, *refs):
    out_ref, *norm_refs = refs[:9]
    held_ref, kept_ref, s_ref, norm_acc, norm_t, sems = refs[9:]
    for i in range(HALO_BLOCKS):

        @pl.when(low_ref[i] < HALO)
        def _():
            part_copy(i, part_ref, kept_ref, sems).start()

    norm_acc[...] = prev_norm[...]
    rows = lambda j: pl.ds(pl.multiple_of(j * TK, TK), TK)
    keys_at = lambda j: halo_ref[rows(j), 0:128]
    values_at = lambda j: halo_ref[rows(j), 128:256]

    def block(i, carry):
        first = pl.multiple_of(i * TQ, TQ)
        j_low = low_ref[i] // TK
        count = HALO // TK - j_low
        row = lax.broadcasted_iota(jnp.int32, (TQ, TK), 0) + (HALO + first)
        lanes = lax.broadcasted_iota(jnp.int32, (TQ, 128), 1)

        @pl.when(count > 0)
        def _():
            part_copy(i, part_ref, kept_ref, sems).wait()

        for blocks in range(1, HALO // TK + 1):

            @pl.when(count == blocks)
            def _():
                q = qkv_ref[pl.ds(first, TQ), 0:256]
                top, total, acc = partial_softmax(
                    q, row, j_low, blocks, False, ends_ref, keys_at, values_at, s_ref
                )
                own = jnp.concatenate(
                    [
                        jnp.sum(
                            jnp.where(lanes == norm_slot(i) + at, norm_acc[...], 0.0),
                            axis=1,
                            keepdims=True,
                        )
                        for at in (0, 2)
                    ],
                    axis=0,
                )
                top = top * SCALE
                most = jnp.maximum(own, top)
                own = jnp.exp(own - most)
                here = jnp.exp(top - most)
                total = own + total * here
                keep(held_ref, i, (kept_ref[i] * own + acc * here) / total)
                keep_norm(norm_acc, i, most + jnp.log(total))
                out_copy(i, held_ref, out_ref, sems).start()

        return carry

    lax.fori_loop(0, HALO_BLOCKS, block, 0)
    norm_t[...] = jnp.transpose(norm_acc[...])
    for d in range(8):
        norm_refs[d][...] = norm_t[pl.ds(pl.multiple_of(((low_ref[BLOCKS] + d) % 8) * 8, 8), 8)]
    for i in range(HALO_BLOCKS):

        @pl.when(low_ref[i] < HALO)
        def _():
            out_copy(i, held_ref, out_ref, sems).wait()


def attend_halo(low, ends, qkv, halo, out, norm, part):
    vmem = pl.BlockSpec(memory_space=pltpu.VMEM)
    any_space = pl.BlockSpec(memory_space=pl.ANY)
    return pl.pallas_call(
        halo_body,
        in_specs=[
            pl.BlockSpec(memory_space=pltpu.SMEM),
            vmem,
            vmem,
            vmem,
            any_space,
            vmem,
            any_space,
        ],
        out_specs=[any_space] + [vmem] * 8,
        out_shape=[jax.ShapeDtypeStruct((SPAN, 256), jnp.bfloat16)]
        + [pltpu.VMEM((8, 128), jnp.float32)] * 8,
        scratch_shapes=[
            pltpu.VMEM((HALO_BLOCKS, TQ, 256), jnp.bfloat16),
            pltpu.VMEM((HALO_BLOCKS, 2 * TQ, 128), jnp.float32),
            pltpu.VMEM((HALO // TK, 2 * TQ, TK), jnp.float32),
            pltpu.VMEM((TQ, 128), jnp.float32),
            pltpu.VMEM((TQ, 128), jnp.float32),
            pltpu.SemaphoreType.DMA((2, HALO_BLOCKS)),
        ],
        input_output_aliases={4: 0},
        name="attend_halo",
    )(low, ends, *in_vmem(qkv, halo), out, norm, part)


def per_device(queries, keys, values, lengths):
    row = lax.axis_index("z")
    base = lax.axis_index("x") * SPAN
    packed = pack(queries, keys, values).reshape(128, 16, 512)
    moved = lax.all_to_all(packed, PLANE, 0, 0, tiled=True)
    low, ends = bounds(lengths, row[None], base[None])
    qkv = moved.reshape(SPAN, 512)
    halo = lax.ppermute(qkv[SPAN - HALO :, 256:512], "x", [(i, i + 1) for i in range(3)])
    out, norm, part = attend_local(low, ends, qkv)
    out, *pieces = attend_halo(low, ends, qkv, halo, out, norm, part)
    back = lax.all_to_all(out.reshape(128, 16, 256), PLANE, 0, 0, tiled=True)
    for d in range(1, 8):
        pieces[d] = lax.ppermute(pieces[d], "z", [(i, (i + d) % 8) for i in range(8)])
    attended, log_norm = unpack(row[None], back.reshape(ROWS, KV_HEADS, 16, 256), pieces)
    return attended, log_norm


def solution(mesh):
    split = Mesh(mesh.devices.reshape(4, 8, 8, 2), ALL)
    wide = P(None, ALL, None)
    return jax.shard_map(
        per_device,
        mesh=split,
        in_specs=(wide, wide, wide, P()),
        out_specs=(wide, P(("y", "c"), None, ("x", "z"))),
        check_vma=False,
    )
```

```python
import jax
import jax.numpy as jnp
from jax import lax
from jax.experimental import pallas as pl
from jax.experimental.pallas import tpu as pltpu
from jax.sharding import Mesh
from jax.sharding import PartitionSpec as P

HEAD = 128
ROWS = 8
KV_HEADS = 16
HALO = 1024
SPAN = 2048
TQ = 256
TK = 256
MOST_BLOCKS = 5
BLOCKS = SPAN // TQ
HALO_BLOCKS = HALO // TQ
FAR = 1 << 20
LOG2E = 1.4426950408889634
SCALE = HEAD ** (-0.5)
ALL = ("x", "z", "y", "c")
PLANE = ("z", "y", "c")


def in_vmem(*arrays):
    return [pltpu.with_memory_space_constraint(a, pltpu.VMEM) for a in arrays]


def doc_bounds(lengths_ref, row, base, low_ref, ends_ref):
    origin = HALO - base
    slot = lax.broadcasted_iota(jnp.int32, (12, TK), 0) * TK
    slot = slot + lax.broadcasted_iota(jnp.int32, (12, TK), 1)
    end = origin
    low = [origin] * BLOCKS
    after = jnp.full((12, TK), FAR, jnp.int32)
    for n in range(32):
        end = end + lengths_ref[row, n]
        low = [jnp.where(end <= HALO + i * TQ, end, low[i]) for i in range(BLOCKS)]
        after = jnp.minimum(after, jnp.where(slot < end, end, FAR))
    ends_ref[...] = jnp.where(slot < origin, 0, after)
    for i in range(BLOCKS):
        low_ref[i] = low[i]
    low_ref[BLOCKS] = row


def bounds_body(lengths_ref, row_ref, base_ref, low_ref, ends_ref):
    doc_bounds(lengths_ref, row_ref[0], base_ref[0], low_ref, ends_ref)


def bounds(lengths, row, base):
    smem = pl.BlockSpec(memory_space=pltpu.SMEM)
    return pl.pallas_call(
        bounds_body,
        in_specs=[smem] * 3,
        out_specs=[smem, pl.BlockSpec(memory_space=pltpu.VMEM)],
        out_shape=[
            jax.ShapeDtypeStruct((BLOCKS + 1,), jnp.int32),
            jax.ShapeDtypeStruct((12, TK), jnp.int32),
        ],
        name="doc_bounds",
    )(lengths, row, base)


def pack_body(q_ref, k_ref, v_ref, out_ref, held_ref, sems):
    parts = ((q_ref, 256, 0), (k_ref, 128, 256), (v_ref, 128, 384))
    reads = [
        [
            pltpu.make_async_copy(
                ref.at[:, :, pl.ds(h * width, width)],
                held_ref.at[:, h, :, pl.ds(at, width)],
                sems.at[n, h],
            )
            for n, (ref, width, at) in enumerate(parts)
        ]
        for h in range(KV_HEADS)
    ]
    writes = [
        pltpu.make_async_copy(held_ref.at[:, h], out_ref.at[:, h], sems.at[3, h])
        for h in range(KV_HEADS)
    ]
    for copies in reads:
        for copy in copies:
            copy.start()
    for h in range(KV_HEADS):
        for copy in reads[h]:
            copy.wait()
        writes[h].start()
    for copy in writes:
        copy.wait()


def pack(queries, keys, values):
    return pl.pallas_call(
        pack_body,
        in_specs=[pl.BlockSpec(memory_space=pl.ANY)] * 3,
        out_specs=pl.BlockSpec(memory_space=pl.ANY),
        out_shape=jax.ShapeDtypeStruct((ROWS, KV_HEADS, 16, 512), jnp.bfloat16),
        scratch_shapes=[
            pltpu.VMEM((ROWS, KV_HEADS, 16, 512), jnp.bfloat16),
            pltpu.SemaphoreType.DMA((4, KV_HEADS)),
        ],
        name="pack",
    )(queries, keys, values)


def unpack_body(row_ref, in_ref, *refs):
    *pieces, out_ref, norm_ref, sems = refs
    copies = [
        pltpu.make_async_copy(
            in_ref.at[:, h], out_ref.at[:, :, pl.ds(h * 256, 256)], sems.at[h]
        )
        for h in range(KV_HEADS)
    ]
    for copy in copies:
        copy.start()
    rows = lax.broadcasted_iota(jnp.int32, (8, 128), 0)
    for h in range(2):
        for n in range(2):
            at = 2 * h + n
            held = jnp.zeros((8, 128), jnp.float32)
            for d in range(8):
                held = jnp.where(rows == (row_ref[0] + 8 - d) % 8, pieces[d][at : at + 1], held)
            norm_ref[h, :, n * 128 : (n + 1) * 128] = held
    for copy in copies:
        copy.wait()


def unpack(row, parts, pieces):
    vmem = pl.BlockSpec(memory_space=pltpu.VMEM)
    return pl.pallas_call(
        unpack_body,
        in_specs=[pl.BlockSpec(memory_space=pltpu.SMEM)] + [vmem] * 9,
        out_specs=[pl.BlockSpec(memory_space=pl.ANY), vmem],
        out_shape=[
            jax.ShapeDtypeStruct((ROWS, 16, 4096), jnp.bfloat16),
            jax.ShapeDtypeStruct((2, ROWS, 256), jnp.float32),
        ],
        scratch_shapes=[pltpu.SemaphoreType.DMA((KV_HEADS,))],
        name="unpack",
    )(row, *in_vmem(parts, *pieces))


def partial_softmax(q, row, j_low, blocks, diagonal, ends_ref, keys_at, values_at, s_ref):
    both = jnp.concatenate((q[:, 0:128], q[:, 128:256]), axis=0)
    top = None
    for n in range(blocks):
        s = lax.dot_general(
            both,
            keys_at(j_low + n),
            (((1,), (1,)), ((), ())),
            preferred_element_type=jnp.float32,
        )
        seen = row < ends_ref[pl.ds(j_low + n, 1), :]
        if diagonal and n == blocks - 1:
            key = lax.broadcasted_iota(jnp.int32, (TQ, TK), 1) + (j_low + n) * TK
            seen = seen & (key <= row)
        halves = []
        for h in range(2):
            part = jnp.where(seen, s[h * TQ : (h + 1) * TQ], -1e30)
            s_ref[n, h * TQ : (h + 1) * TQ] = part
            halves.append(jnp.maximum(part[:, 0:128], part[:, 128:256]))
        here = jnp.concatenate(halves, axis=0)
        top = here if top is None else jnp.maximum(top, here)
    top = jnp.max(top, axis=1, keepdims=True)
    total = acc = None
    for n in range(blocks):
        w = jnp.exp2((s_ref[n] - top) * (SCALE * LOG2E))
        part = w[:, 0:128] + w[:, 128:256]
        o = jnp.dot(
            w.astype(jnp.bfloat16), values_at(j_low + n), preferred_element_type=jnp.float32
        )
        total = part if total is None else total + part
        acc = o if acc is None else acc + o
    return top, jnp.sum(total, axis=1, keepdims=True), acc


def out_copy(i, held_ref, out_ref, sems):
    return pltpu.make_async_copy(held_ref.at[i], out_ref.at[pl.ds(i * TQ, TQ)], sems.at[0, i])


def part_copy(i, src_ref, dst_ref, sems):
    return pltpu.make_async_copy(src_ref.at[i], dst_ref.at[i], sems.at[1, i])


def keep(held_ref, i, result):
    result = result.astype(jnp.bfloat16)
    held_ref[i, :, 0:128] = result[0:TQ]
    held_ref[i, :, 128:256] = result[TQ : 2 * TQ]


def norm_lanes(i):
    return [(8 * i + n, slice(n * 128, (n + 1) * 128)) for n in range(4)]


def keep_norm(norm_acc, i, norm):
    lanes = lax.broadcasted_iota(jnp.int32, (128, 128), 1)
    held = norm_acc[...]
    for lane, rows in norm_lanes(i):
        held = jnp.where(lanes == lane, norm[rows], held)
    norm_acc[...] = held


def kept_norm(norm_acc, i):
    lanes = lax.broadcasted_iota(jnp.int32, (128, 128), 1)
    held = norm_acc[...]
    return jnp.concatenate(
        [
            jnp.sum(jnp.where(lanes == lane, held, 0.0), axis=1, keepdims=True)
            for lane, _ in norm_lanes(i)
        ],
        axis=0,
    )


def local_body(
    low_ref, ends_ref, qkv_ref, out_ref, norm_ref, part_ref, held_ref, kept_ref, s_ref, sems
):
    norm_ref[...] = jnp.zeros((128, 128), jnp.float32)
    rows = lambda j: pl.ds(pl.multiple_of(j * TK - HALO, TK), TK)
    keys_at = lambda j: qkv_ref[rows(j), 256:384]
    values_at = lambda j: qkv_ref[rows(j), 384:512]

    def block(i, carry):
        first = pl.multiple_of(i * TQ, TQ)
        j_low = jnp.maximum(low_ref[i], HALO) // TK
        count = (HALO + first) // TK + 1 - j_low
        row = lax.broadcasted_iota(jnp.int32, (TQ, TK), 0) + (HALO + first)
        for blocks in range(1, MOST_BLOCKS + 1):

            @pl.when(count == blocks)
            def _():
                q = qkv_ref[pl.ds(first, TQ), 0:256]
                top, total, acc = partial_softmax(
                    q, row, j_low, blocks, True, ends_ref, keys_at, values_at, s_ref
                )
                result = acc / total
                kept_ref[i] = result
                keep(held_ref, i, result)
                keep_norm(norm_ref, i, top * SCALE + jnp.log(total))

        @pl.when(low_ref[i] >= HALO)
        def _():
            out_copy(i, held_ref, out_ref, sems).start()

        @pl.when(low_ref[i] < HALO)
        def _():
            part_copy(i, kept_ref, part_ref, sems).start()

        return carry

    lax.fori_loop(0, BLOCKS, block, 0)
    for i in range(BLOCKS):

        @pl.when(low_ref[i] >= HALO)
        def _():
            out_copy(i, held_ref, out_ref, sems).wait()

        if i < HALO_BLOCKS:

            @pl.when(low_ref[i] < HALO)
            def _():
                part_copy(i, kept_ref, part_ref, sems).wait()


def attend_local(low, ends, qkv):
    vmem = pl.BlockSpec(memory_space=pltpu.VMEM)
    any_space = pl.BlockSpec(memory_space=pl.ANY)
    return pl.pallas_call(
        local_body,
        in_specs=[pl.BlockSpec(memory_space=pltpu.SMEM), vmem, vmem],
        out_specs=[any_space, vmem, any_space],
        out_shape=[
            jax.ShapeDtypeStruct((SPAN, 256), jnp.bfloat16),
            jax.ShapeDtypeStruct((128, 128), jnp.float32),
            jax.ShapeDtypeStruct((HALO_BLOCKS, 2 * TQ, 128), jnp.float32),
        ],
        scratch_shapes=[
            pltpu.VMEM((BLOCKS, TQ, 256), jnp.bfloat16),
            pltpu.VMEM((BLOCKS, 2 * TQ, 128), jnp.float32),
            pltpu.VMEM((MOST_BLOCKS, 2 * TQ, TK), jnp.float32),
            pltpu.SemaphoreType.DMA((2, BLOCKS)),
        ],
        name="attend_local",
    )(low, ends, *in_vmem(qkv))


def halo_body(low_ref, ends_ref, qkv_ref, halo_ref, prev_ref, prev_norm, part_ref, *refs):
    out_ref, *norm_refs = refs[:9]
    held_ref, kept_ref, s_ref, norm_acc, norm_t, sems = refs[9:]
    for i in range(HALO_BLOCKS):

        @pl.when(low_ref[i] < HALO)
        def _():
            part_copy(i, part_ref, kept_ref, sems).start()

    norm_acc[...] = prev_norm[...]
    rows = lambda j: pl.ds(pl.multiple_of(j * TK, TK), TK)
    keys_at = lambda j: halo_ref[rows(j), 0:128]
    values_at = lambda j: halo_ref[rows(j), 128:256]

    def block(i, carry):
        first = pl.multiple_of(i * TQ, TQ)
        j_low = low_ref[i] // TK
        count = HALO // TK - j_low
        row = lax.broadcasted_iota(jnp.int32, (TQ, TK), 0) + (HALO + first)

        for blocks in range(1, HALO // TK + 1):

            @pl.when(count == blocks)
            def _():
                q = qkv_ref[pl.ds(first, TQ), 0:256]
                top, total, acc = partial_softmax(
                    q, row, j_low, blocks, False, ends_ref, keys_at, values_at, s_ref
                )
                own = kept_norm(norm_acc, i)
                part_copy(i, part_ref, kept_ref, sems).wait()
                top = top * SCALE
                most = jnp.maximum(own, top)
                own = jnp.exp(own - most)
                here = jnp.exp(top - most)
                total = own + total * here
                keep(held_ref, i, (kept_ref[i] * own + acc * here) / total)
                keep_norm(norm_acc, i, most + jnp.log(total))
                out_copy(i, held_ref, out_ref, sems).start()

        return carry

    lax.fori_loop(0, HALO_BLOCKS, block, 0)
    norm_t[...] = jnp.transpose(norm_acc[...])
    for d in range(8):
        norm_refs[d][...] = norm_t[pl.ds(pl.multiple_of(((low_ref[BLOCKS] + d) % 8) * 8, 8), 8)]
    for i in range(HALO_BLOCKS):

        @pl.when(low_ref[i] < HALO)
        def _():
            out_copy(i, held_ref, out_ref, sems).wait()


def attend_halo(low, ends, qkv, halo, out, norm, part):
    vmem = pl.BlockSpec(memory_space=pltpu.VMEM)
    any_space = pl.BlockSpec(memory_space=pl.ANY)
    return pl.pallas_call(
        halo_body,
        in_specs=[
            pl.BlockSpec(memory_space=pltpu.SMEM),
            vmem,
            vmem,
            vmem,
            any_space,
            vmem,
            any_space,
        ],
        out_specs=[any_space] + [vmem] * 8,
        out_shape=[jax.ShapeDtypeStruct((SPAN, 256), jnp.bfloat16)]
        + [pltpu.VMEM((8, 128), jnp.float32)] * 8,
        scratch_shapes=[
            pltpu.VMEM((HALO_BLOCKS, TQ, 256), jnp.bfloat16),
            pltpu.VMEM((HALO_BLOCKS, 2 * TQ, 128), jnp.float32),
            pltpu.VMEM((HALO // TK, 2 * TQ, TK), jnp.float32),
            pltpu.VMEM((128, 128), jnp.float32),
            pltpu.VMEM((128, 128), jnp.float32),
            pltpu.SemaphoreType.DMA((2, HALO_BLOCKS)),
        ],
        input_output_aliases={4: 0},
        name="attend_halo",
    )(low, ends, *in_vmem(qkv, halo), out, norm, part)


def per_device(queries, keys, values, lengths):
    row = lax.axis_index("z")
    base = lax.axis_index("x") * SPAN
    packed = pack(queries, keys, values).reshape(128, 16, 512)
    moved = lax.all_to_all(packed, PLANE, 0, 0, tiled=True)
    low, ends = bounds(lengths, row[None], base[None])
    qkv = moved.reshape(SPAN, 512)
    halo = lax.ppermute(qkv[SPAN - HALO :, 256:512], "x", [(i, i + 1) for i in range(3)])
    out, norm, part = attend_local(low, ends, qkv)
    out, *pieces = attend_halo(low, ends, qkv, halo, out, norm, part)
    back = lax.all_to_all(out.reshape(128, 16, 256), PLANE, 0, 0, tiled=True)
    for d in range(1, 8):
        pieces[d] = lax.ppermute(pieces[d], "z", [(i, (i + d) % 8) for i in range(8)])
    attended, log_norm = unpack(row[None], back.reshape(ROWS, KV_HEADS, 16, 256), pieces)
    return attended, log_norm


def solution(mesh):
    split = Mesh(mesh.devices.reshape(4, 8, 8, 2), ALL)
    wide = P(None, ALL, None)
    return jax.shard_map(
        per_device,
        mesh=split,
        in_specs=(wide, wide, wide, P()),
        out_specs=(wide, P(("y", "c"), None, ("x", "z"))),
        check_vma=False,
    )
```

```python
import jax
import jax.numpy as jnp
from jax import lax
from jax.experimental import pallas as pl
from jax.experimental.pallas import tpu as pltpu
from jax.sharding import Mesh
from jax.sharding import PartitionSpec as P

HEAD = 128
ROWS = 8
KV_HEADS = 16
HALO = 1024
SPAN = 2048
TQ = 256
TK = 256
MOST_BLOCKS = 5
BLOCKS = SPAN // TQ
HALO_BLOCKS = HALO // TQ
FAR = 1 << 20
LOG2E = 1.4426950408889634
SCALE = HEAD ** (-0.5)
ALL = ("x", "z", "y", "c")
PLANE = ("z", "y", "c")


def in_vmem(*arrays):
    return [pltpu.with_memory_space_constraint(a, pltpu.VMEM) for a in arrays]


def doc_bounds(lengths_ref, row, base, low_ref, ends_ref):
    origin = HALO - base
    slot = lax.broadcasted_iota(jnp.int32, (12, TK), 0) * TK
    slot = slot + lax.broadcasted_iota(jnp.int32, (12, TK), 1)
    end = origin
    low = [origin] * BLOCKS
    after = jnp.full((12, TK), FAR, jnp.int32)
    for n in range(32):
        end = end + lengths_ref[row, n]
        low = [jnp.where(end <= HALO + i * TQ, end, low[i]) for i in range(BLOCKS)]
        after = jnp.minimum(after, jnp.where(slot < end, end, FAR))
    ends_ref[...] = jnp.where(slot < origin, 0, after)
    for i in range(BLOCKS):
        low_ref[i] = low[i]
    low_ref[BLOCKS] = row


def bounds_body(lengths_ref, row_ref, base_ref, low_ref, ends_ref):
    doc_bounds(lengths_ref, row_ref[0], base_ref[0], low_ref, ends_ref)


def bounds(lengths, row, base):
    smem = pl.BlockSpec(memory_space=pltpu.SMEM)
    return pl.pallas_call(
        bounds_body,
        in_specs=[smem] * 3,
        out_specs=[smem, pl.BlockSpec(memory_space=pltpu.VMEM)],
        out_shape=[
            jax.ShapeDtypeStruct((BLOCKS + 1,), jnp.int32),
            jax.ShapeDtypeStruct((12, TK), jnp.int32),
        ],
        name="doc_bounds",
    )(lengths, row, base)


def pack_body(q_ref, k_ref, v_ref, out_ref, held_ref, sems):
    parts = ((q_ref, 256, 0), (k_ref, 128, 256), (v_ref, 128, 384))
    reads = [
        [
            pltpu.make_async_copy(
                ref.at[:, :, pl.ds(h * width, width)],
                held_ref.at[:, h, :, pl.ds(at, width)],
                sems.at[n, h],
            )
            for n, (ref, width, at) in enumerate(parts)
        ]
        for h in range(KV_HEADS)
    ]
    writes = [
        pltpu.make_async_copy(held_ref.at[:, h], out_ref.at[:, h], sems.at[3, h])
        for h in range(KV_HEADS)
    ]
    for copies in reads:
        for copy in copies:
            copy.start()
    for h in range(KV_HEADS):
        for copy in reads[h]:
            copy.wait()
        writes[h].start()
    for copy in writes:
        copy.wait()


def pack(queries, keys, values):
    return pl.pallas_call(
        pack_body,
        in_specs=[pl.BlockSpec(memory_space=pl.ANY)] * 3,
        out_specs=pl.BlockSpec(memory_space=pl.ANY),
        out_shape=jax.ShapeDtypeStruct((ROWS, KV_HEADS, 16, 512), jnp.bfloat16),
        scratch_shapes=[
            pltpu.VMEM((ROWS, KV_HEADS, 16, 512), jnp.bfloat16),
            pltpu.SemaphoreType.DMA((4, KV_HEADS)),
        ],
        name="pack",
    )(queries, keys, values)


def unpack_body(row_ref, in_ref, *refs):
    *pieces, out_ref, norm_out, norm_ref, sems, norm_sem = refs
    copies = [
        pltpu.make_async_copy(
            in_ref.at[:, h], out_ref.at[:, :, pl.ds(h * 256, 256)], sems.at[h]
        )
        for h in range(KV_HEADS)
    ]
    for copy in copies:
        copy.start()
    rows = lax.broadcasted_iota(jnp.int32, (8, 128), 0)
    for h in range(2):
        for n in range(2):
            at = 2 * h + n
            held = jnp.zeros((8, 128), jnp.float32)
            for d in range(8):
                held = jnp.where(rows == (row_ref[0] + 8 - d) % 8, pieces[d][at : at + 1], held)
            norm_ref[h, :, n * 128 : (n + 1) * 128] = held
    norm_copy = pltpu.make_async_copy(norm_ref, norm_out, norm_sem)
    norm_copy.start()
    norm_copy.wait()
    for copy in copies:
        copy.wait()


def unpack(row, parts, pieces):
    vmem = pl.BlockSpec(memory_space=pltpu.VMEM)
    return pl.pallas_call(
        unpack_body,
        in_specs=[pl.BlockSpec(memory_space=pltpu.SMEM)] + [vmem] * 9,
        out_specs=[pl.BlockSpec(memory_space=pl.ANY)] * 2,
        out_shape=[
            jax.ShapeDtypeStruct((ROWS, 16, 4096), jnp.bfloat16),
            jax.ShapeDtypeStruct((2, ROWS, 256), jnp.float32),
        ],
        scratch_shapes=[
            pltpu.VMEM((2, ROWS, 256), jnp.float32),
            pltpu.SemaphoreType.DMA((KV_HEADS,)),
            pltpu.SemaphoreType.DMA,
        ],
        name="unpack",
    )(row, *in_vmem(parts, *pieces))


def partial_softmax(parts, rows, j_low, blocks, diagonal, ends_ref, keys_at, values_at, s_ref):
    tops, totals, accs = [], [], []
    for p in range(len(parts)):
        at, row, top = slice(p * TQ, (p + 1) * TQ), rows[p // 2], None
        for n in range(blocks):
            s = lax.dot_general(
                parts[p],
                keys_at(j_low + n),
                (((1,), (1,)), ((), ())),
                preferred_element_type=jnp.float32,
            )
            seen = row < ends_ref[pl.ds(j_low + n, 1), :]
            if diagonal and n == blocks - 1:
                key = lax.broadcasted_iota(jnp.int32, (TQ, TK), 1) + (j_low + n) * TK
                seen = seen & (key <= row)
            s = jnp.where(seen, s, -1e30)
            s_ref[n, at] = s
            here = jnp.maximum(s[:, 0:128], s[:, 128:256])
            top = here if top is None else jnp.maximum(top, here)
        tops.append(jnp.broadcast_to(jnp.max(top, axis=1, keepdims=True), top.shape))
    for p in range(len(parts)):
        at, total, acc = slice(p * TQ, (p + 1) * TQ), None, None
        top = jnp.concatenate((tops[p], tops[p]), axis=1)
        for n in range(blocks):
            w = jnp.exp2((s_ref[n, at] - top) * (SCALE * LOG2E))
            part = w[:, 0:128] + w[:, 128:256]
            o = jnp.dot(
                w.astype(jnp.bfloat16), values_at(j_low + n), preferred_element_type=jnp.float32
            )
            total = part if total is None else total + part
            acc = o if acc is None else acc + o
        lead = total.astype(jnp.bfloat16)
        trail = (total - lead.astype(jnp.float32)).astype(jnp.bfloat16)
        totals.append(
            jnp.dot(
                jnp.concatenate((lead, trail), axis=1),
                jnp.ones((256, 128), jnp.bfloat16),
                preferred_element_type=jnp.float32,
            )
        )
        accs.append(acc)
    return tuple(jnp.concatenate(v, axis=0) for v in (tops, totals, accs))


def head_parts(qkv_ref, i):
    q = qkv_ref[pl.ds(pl.multiple_of(i * TQ, TQ), TQ), 0:256]
    return [q[:, 0:128], q[:, 128:256]]


def positions(i):
    return lax.broadcasted_iota(jnp.int32, (TQ, TK), 0) + (HALO + i * TQ)


def out_copy(i, held_ref, out_ref, sems):
    return pltpu.make_async_copy(held_ref.at[i], out_ref.at[pl.ds(i * TQ, TQ)], sems.at[0, i])


def part_copy(i, src_ref, dst_ref, sems):
    return pltpu.make_async_copy(src_ref.at[i], dst_ref.at[i], sems.at[1, i])


def keep(held_ref, i, result):
    result = result.astype(jnp.bfloat16)
    held_ref[i, :, 0:128] = result[0:TQ]
    held_ref[i, :, 128:256] = result[TQ : 2 * TQ]


def norm_lanes(i):
    return [(8 * i + n, slice(n * 128, (n + 1) * 128)) for n in range(4)]


def keep_norm(norm_acc, i, norm):
    lanes = lax.broadcasted_iota(jnp.int32, (128, 128), 1)
    held = norm_acc[...]
    for lane, rows in norm_lanes(i):
        held = jnp.where(lanes == lane, norm[rows], held)
    norm_acc[...] = held


def local_body(
    low_ref, ends_ref, qkv_ref, out_ref, norm_ref, part_ref, held_ref, kept_ref, s_ref, sems
):
    norm_ref[...] = jnp.zeros((128, 128), jnp.float32)
    rows = lambda j: pl.ds(pl.multiple_of(j * TK - HALO, TK), TK)
    keys_at = lambda j: qkv_ref[rows(j), 256:384]
    values_at = lambda j: qkv_ref[rows(j), 384:512]

    def block(i, carry):
        first = pl.multiple_of(i * TQ, TQ)
        j_low = jnp.maximum(low_ref[i], HALO) // TK
        count = (HALO + first) // TK + 1 - j_low
        parts, row = head_parts(qkv_ref, i), positions(i)
        for blocks in range(1, MOST_BLOCKS + 1):

            @pl.when(count == blocks)
            def _():
                top, total, acc = partial_softmax(
                    parts, [row], j_low, blocks, True, ends_ref, keys_at, values_at, s_ref
                )
                result = acc / total
                norm = top * SCALE + jnp.log(total)
                kept_ref[i, 0] = result
                kept_ref[i, 1] = norm
                keep(held_ref, i, result)
                keep_norm(norm_ref, i, norm)

        pair_low = low_ref[i // 2 * 2]

        @pl.when(pair_low >= HALO)
        def _():
            out_copy(i, held_ref, out_ref, sems).start()

        @pl.when(pair_low < HALO)
        def _():
            part_copy(i, kept_ref, part_ref, sems).start()

        return carry

    lax.fori_loop(0, BLOCKS, block, 0)
    for i in range(BLOCKS):

        @pl.when(low_ref[i // 2 * 2] >= HALO)
        def _():
            out_copy(i, held_ref, out_ref, sems).wait()

        if i < HALO_BLOCKS:

            @pl.when(low_ref[i // 2 * 2] < HALO)
            def _():
                part_copy(i, kept_ref, part_ref, sems).wait()


def attend_local(low, ends, qkv):
    vmem = pl.BlockSpec(memory_space=pltpu.VMEM)
    any_space = pl.BlockSpec(memory_space=pl.ANY)
    return pl.pallas_call(
        local_body,
        in_specs=[pl.BlockSpec(memory_space=pltpu.SMEM), vmem, vmem],
        out_specs=[any_space, vmem, any_space],
        out_shape=[
            jax.ShapeDtypeStruct((SPAN, 256), jnp.bfloat16),
            jax.ShapeDtypeStruct((128, 128), jnp.float32),
            jax.ShapeDtypeStruct((HALO_BLOCKS, 2, 2 * TQ, 128), jnp.float32),
        ],
        scratch_shapes=[
            pltpu.VMEM((BLOCKS, TQ, 256), jnp.bfloat16),
            pltpu.VMEM((BLOCKS, 2, 2 * TQ, 128), jnp.float32),
            pltpu.VMEM((MOST_BLOCKS, 2 * TQ, TK), jnp.float32),
            pltpu.SemaphoreType.DMA((2, BLOCKS)),
        ],
        name="attend_local",
    )(low, ends, *in_vmem(qkv))


def halo_body(low_ref, ends_ref, qkv_ref, halo_ref, prev_ref, prev_norm, part_ref, *refs):
    out_ref, *norm_refs = refs[:9]
    held_ref, kept_ref, s_ref, norm_acc, norm_t, sems = refs[9:]
    for i in range(HALO_BLOCKS):

        @pl.when(low_ref[i // 2 * 2] < HALO)
        def _():
            part_copy(i, part_ref, kept_ref, sems).start()

    norm_acc[...] = prev_norm[...]
    rows = lambda j: pl.ds(pl.multiple_of(j * TK, TK), TK)
    keys_at = lambda j: halo_ref[rows(j), 0:128]
    values_at = lambda j: halo_ref[rows(j), 128:256]

    def pair(p, carry):
        pair_blocks = (2 * p, 2 * p + 1)
        j_low = low_ref[2 * p] // TK
        count = HALO // TK - j_low
        for blocks in range(1, HALO // TK + 1):

            @pl.when(count == blocks)
            def _():
                top, total, acc = partial_softmax(
                    [part for i in pair_blocks for part in head_parts(qkv_ref, i)],
                    [positions(i) for i in pair_blocks],
                    j_low,
                    blocks,
                    False,
                    ends_ref,
                    keys_at,
                    values_at,
                    s_ref,
                )
                for i in pair_blocks:
                    part_copy(i, part_ref, kept_ref, sems).wait()
                for n, i in enumerate(pair_blocks):
                    at = slice(2 * n * TQ, 2 * (n + 1) * TQ)
                    own, these = kept_ref[i, 1], top[at] * SCALE
                    most = jnp.maximum(own, these)
                    own, these = jnp.exp(own - most), jnp.exp(these - most)
                    whole = own + total[at] * these
                    keep(held_ref, i, (kept_ref[i, 0] * own + acc[at] * these) / whole)
                    out_copy(i, held_ref, out_ref, sems).start()
                    keep_norm(norm_acc, i, most + jnp.log(whole))

        return carry

    lax.fori_loop(0, HALO_BLOCKS // 2, pair, 0)
    norm_t[...] = jnp.transpose(norm_acc[...])
    for d in range(8):
        norm_refs[d][...] = norm_t[pl.ds(pl.multiple_of(((low_ref[BLOCKS] + d) % 8) * 8, 8), 8)]
    for i in range(HALO_BLOCKS):

        @pl.when(low_ref[i // 2 * 2] < HALO)
        def _():
            out_copy(i, held_ref, out_ref, sems).wait()


def attend_halo(low, ends, qkv, halo, out, norm, part):
    vmem = pl.BlockSpec(memory_space=pltpu.VMEM)
    any_space = pl.BlockSpec(memory_space=pl.ANY)
    return pl.pallas_call(
        halo_body,
        in_specs=[
            pl.BlockSpec(memory_space=pltpu.SMEM),
            vmem,
            vmem,
            vmem,
            any_space,
            vmem,
            any_space,
        ],
        out_specs=[any_space] + [vmem] * 8,
        out_shape=[jax.ShapeDtypeStruct((SPAN, 256), jnp.bfloat16)]
        + [pltpu.VMEM((8, 128), jnp.float32)] * 8,
        scratch_shapes=[
            pltpu.VMEM((HALO_BLOCKS, TQ, 256), jnp.bfloat16),
            pltpu.VMEM((HALO_BLOCKS, 2, 2 * TQ, 128), jnp.float32),
            pltpu.VMEM((HALO // TK, 4 * TQ, TK), jnp.float32),
            pltpu.VMEM((128, 128), jnp.float32),
            pltpu.VMEM((128, 128), jnp.float32),
            pltpu.SemaphoreType.DMA((2, HALO_BLOCKS)),
        ],
        input_output_aliases={4: 0},
        name="attend_halo",
    )(low, ends, *in_vmem(qkv, halo), out, norm, part)


def per_device(queries, keys, values, lengths):
    row = lax.axis_index("z")
    base = lax.axis_index("x") * SPAN
    packed = pack(queries, keys, values).reshape(128, 16, 512)
    moved = lax.all_to_all(packed, PLANE, 0, 0, tiled=True)
    low, ends = bounds(lengths, row[None], base[None])
    qkv = moved.reshape(SPAN, 512)
    halo = lax.ppermute(qkv[SPAN - HALO :, 256:512], "x", [(i, i + 1) for i in range(3)])
    out, norm, part = attend_local(low, ends, qkv)
    out, *pieces = attend_halo(low, ends, qkv, halo, out, norm, part)
    back = lax.all_to_all(out.reshape(128, 16, 256), PLANE, 0, 0, tiled=True)
    for d in range(1, 8):
        pieces[d] = lax.ppermute(pieces[d], "z", [(i, (i + d) % 8) for i in range(8)])
    attended, log_norm = unpack(row[None], back.reshape(ROWS, KV_HEADS, 16, 256), pieces)
    return attended, log_norm


def solution(mesh):
    split = Mesh(mesh.devices.reshape(4, 8, 8, 2), ALL)
    wide = P(None, ALL, None)
    return jax.shard_map(
        per_device,
        mesh=split,
        in_specs=(wide, wide, wide, P()),
        out_specs=(wide, P(("y", "c"), None, ("x", "z"))),
        check_vma=False,
    )
```

```python
import jax
import jax.numpy as jnp
from jax import lax
from jax.experimental import pallas as pl
from jax.experimental.pallas import tpu as pltpu
from jax.sharding import Mesh
from jax.sharding import PartitionSpec as P

HEAD = 128
ROWS = 8
KV_HEADS = 16
HALO = 1024
SPAN = 2048
TQ = 256
TK = 256
MOST_BLOCKS = 5
BLOCKS = SPAN // TQ
HALO_BLOCKS = HALO // TQ
FAR = 1 << 20
LOG2E = 1.4426950408889634
SCALE = HEAD ** (-0.5)
ALL = ("x", "z", "y", "c")
PLANE = ("z", "y", "c")


def in_vmem(*arrays):
    return [pltpu.with_memory_space_constraint(a, pltpu.VMEM) for a in arrays]


def doc_bounds(lengths_ref, row, base, low_ref, ends_ref):
    origin = HALO - base
    slot = lax.broadcasted_iota(jnp.int32, (12, TK), 0) * TK
    slot = slot + lax.broadcasted_iota(jnp.int32, (12, TK), 1)
    end = origin
    low = [origin] * BLOCKS
    after = jnp.full((12, TK), FAR, jnp.int32)
    for n in range(32):
        end = end + lengths_ref[row, n]
        low = [jnp.where(end <= HALO + i * TQ, end, low[i]) for i in range(BLOCKS)]
        after = jnp.minimum(after, jnp.where(slot < end, end, FAR))
    ends_ref[...] = jnp.where(slot < origin, 0, after)
    for i in range(BLOCKS):
        low_ref[i] = low[i]
    low_ref[BLOCKS] = row


def bounds_body(lengths_ref, row_ref, base_ref, low_ref, ends_ref):
    doc_bounds(lengths_ref, row_ref[0], base_ref[0], low_ref, ends_ref)


def bounds(lengths, row, base):
    smem = pl.BlockSpec(memory_space=pltpu.SMEM)
    return pl.pallas_call(
        bounds_body,
        in_specs=[smem] * 3,
        out_specs=[smem, pl.BlockSpec(memory_space=pltpu.VMEM)],
        out_shape=[
            jax.ShapeDtypeStruct((BLOCKS + 1,), jnp.int32),
            jax.ShapeDtypeStruct((12, TK), jnp.int32),
        ],
        name="doc_bounds",
    )(lengths, row, base)


def pack_body(q_ref, k_ref, v_ref, out_ref, held_ref, sems):
    parts = ((q_ref, 256, 0), (k_ref, 128, 256), (v_ref, 128, 384))
    reads = [
        [
            pltpu.make_async_copy(
                ref.at[:, :, pl.ds(h * width, width)],
                held_ref.at[:, h, :, pl.ds(at, width)],
                sems.at[n, h],
            )
            for n, (ref, width, at) in enumerate(parts)
        ]
        for h in range(KV_HEADS)
    ]
    writes = [
        pltpu.make_async_copy(held_ref.at[:, h], out_ref.at[:, h], sems.at[3, h])
        for h in range(KV_HEADS)
    ]
    for copies in reads:
        for copy in copies:
            copy.start()
    for h in range(KV_HEADS):
        for copy in reads[h]:
            copy.wait()
        writes[h].start()
    for copy in writes:
        copy.wait()


def pack(queries, keys, values):
    return pl.pallas_call(
        pack_body,
        in_specs=[pl.BlockSpec(memory_space=pl.ANY)] * 3,
        out_specs=pl.BlockSpec(memory_space=pl.ANY),
        out_shape=jax.ShapeDtypeStruct((ROWS, KV_HEADS, 16, 512), jnp.bfloat16),
        scratch_shapes=[
            pltpu.VMEM((ROWS, KV_HEADS, 16, 512), jnp.bfloat16),
            pltpu.SemaphoreType.DMA((4, KV_HEADS)),
        ],
        name="pack",
    )(queries, keys, values)


def unpack_body(row_ref, in_ref, *refs):
    *pieces, out_ref, norm_out, norm_ref, sems, norm_sem = refs
    copies = [
        pltpu.make_async_copy(
            in_ref.at[:, h], out_ref.at[:, :, pl.ds(h * 256, 256)], sems.at[h]
        )
        for h in range(KV_HEADS)
    ]
    for copy in copies:
        copy.start()
    rows = lax.broadcasted_iota(jnp.int32, (8, 128), 0)
    for h in range(2):
        for n in range(2):
            at = 2 * h + n
            held = jnp.zeros((8, 128), jnp.float32)
            for d in range(8):
                held = jnp.where(rows == (row_ref[0] + 8 - d) % 8, pieces[d % 4][d // 4, at : at + 1], held)
            norm_ref[h, :, n * 128 : (n + 1) * 128] = held
    norm_copy = pltpu.make_async_copy(norm_ref, norm_out, norm_sem)
    norm_copy.start()
    norm_copy.wait()
    for copy in copies:
        copy.wait()


def unpack(row, parts, pairs):
    vmem = pl.BlockSpec(memory_space=pltpu.VMEM)
    return pl.pallas_call(
        unpack_body,
        in_specs=[pl.BlockSpec(memory_space=pltpu.SMEM)] + [vmem] * 5,
        out_specs=[pl.BlockSpec(memory_space=pl.ANY)] * 2,
        out_shape=[
            jax.ShapeDtypeStruct((ROWS, 16, 4096), jnp.bfloat16),
            jax.ShapeDtypeStruct((2, ROWS, 256), jnp.float32),
        ],
        scratch_shapes=[
            pltpu.VMEM((2, ROWS, 256), jnp.float32),
            pltpu.SemaphoreType.DMA((KV_HEADS,)),
            pltpu.SemaphoreType.DMA,
        ],
        name="unpack",
    )(row, *in_vmem(parts, *pairs))


def partial_softmax(parts, rows, j_low, blocks, diagonal, ends_ref, keys_at, values_at, s_ref):
    tops, totals, accs = [], [], []
    for p in range(len(parts)):
        at, row, top = slice(p * TQ, (p + 1) * TQ), rows[p // 2], None
        for n in range(blocks):
            s = lax.dot_general(
                parts[p],
                keys_at(j_low + n),
                (((1,), (1,)), ((), ())),
                preferred_element_type=jnp.float32,
            )
            seen = row < ends_ref[pl.ds(j_low + n, 1), :]
            if diagonal and n == blocks - 1:
                key = lax.broadcasted_iota(jnp.int32, (TQ, TK), 1) + (j_low + n) * TK
                seen = seen & (key <= row)
            s = jnp.where(seen, s, -1e30)
            s_ref[n, at] = s
            here = jnp.maximum(s[:, 0:128], s[:, 128:256])
            top = here if top is None else jnp.maximum(top, here)
        tops.append(jnp.broadcast_to(jnp.max(top, axis=1, keepdims=True), top.shape))
    for p in range(len(parts)):
        at, total, acc = slice(p * TQ, (p + 1) * TQ), None, None
        top = jnp.concatenate((tops[p], tops[p]), axis=1)
        for n in range(blocks):
            w = jnp.exp2((s_ref[n, at] - top) * (SCALE * LOG2E))
            part = w[:, 0:128] + w[:, 128:256]
            o = jnp.dot(
                w.astype(jnp.bfloat16), values_at(j_low + n), preferred_element_type=jnp.float32
            )
            total = part if total is None else total + part
            acc = o if acc is None else acc + o
        lead = total.astype(jnp.bfloat16)
        trail = (total - lead.astype(jnp.float32)).astype(jnp.bfloat16)
        totals.append(
            jnp.dot(
                jnp.concatenate((lead, trail), axis=1),
                jnp.ones((256, 128), jnp.bfloat16),
                preferred_element_type=jnp.float32,
            )
        )
        accs.append(acc)
    return tuple(jnp.concatenate(v, axis=0) for v in (tops, totals, accs))


def head_parts(qkv_ref, i):
    q = qkv_ref[pl.ds(pl.multiple_of(i * TQ, TQ), TQ), 0:256]
    return [q[:, 0:128], q[:, 128:256]]


def positions(i):
    return lax.broadcasted_iota(jnp.int32, (TQ, TK), 0) + (HALO + i * TQ)


def out_copy(i, held_ref, out_ref, sems):
    return pltpu.make_async_copy(held_ref.at[i], out_ref.at[pl.ds(i * TQ, TQ)], sems.at[0, i])


def part_copy(i, src_ref, dst_ref, sems):
    return pltpu.make_async_copy(src_ref.at[i], dst_ref.at[i], sems.at[1, i])


def keep(held_ref, i, result):
    result = result.astype(jnp.bfloat16)
    held_ref[i, :, 0:128] = result[0:TQ]
    held_ref[i, :, 128:256] = result[TQ : 2 * TQ]


def norm_lanes(i):
    return [(8 * i + n, slice(n * 128, (n + 1) * 128)) for n in range(4)]


def keep_norm(norm_acc, i, norm):
    lanes = lax.broadcasted_iota(jnp.int32, (128, 128), 1)
    held = norm_acc[...]
    for lane, rows in norm_lanes(i):
        held = jnp.where(lanes == lane, norm[rows], held)
    norm_acc[...] = held


def local_body(
    low_ref, ends_ref, qkv_ref, out_ref, norm_ref, part_ref, held_ref, kept_ref, s_ref, sems
):
    norm_ref[...] = jnp.zeros((128, 128), jnp.float32)
    rows = lambda j: pl.ds(pl.multiple_of(j * TK - HALO, TK), TK)
    keys_at = lambda j: qkv_ref[rows(j), 256:384]
    values_at = lambda j: qkv_ref[rows(j), 384:512]

    def block(i, carry):
        first = pl.multiple_of(i * TQ, TQ)
        j_low = jnp.maximum(low_ref[i], HALO) // TK
        count = (HALO + first) // TK + 1 - j_low
        parts, row = head_parts(qkv_ref, i), positions(i)
        for blocks in range(1, MOST_BLOCKS + 1):

            @pl.when(count == blocks)
            def _():
                top, total, acc = partial_softmax(
                    parts, [row], j_low, blocks, True, ends_ref, keys_at, values_at, s_ref
                )
                result = acc / total
                norm = top * SCALE + jnp.log(total)
                kept_ref[i, 0] = result
                kept_ref[i, 1] = norm
                keep(held_ref, i, result)
                keep_norm(norm_ref, i, norm)

        pair_low = low_ref[i // 2 * 2]

        @pl.when(pair_low >= HALO)
        def _():
            out_copy(i, held_ref, out_ref, sems).start()

        @pl.when(pair_low < HALO)
        def _():
            part_copy(i, kept_ref, part_ref, sems).start()

        return carry

    lax.fori_loop(0, BLOCKS, block, 0)
    for i in range(BLOCKS):

        @pl.when(low_ref[i // 2 * 2] >= HALO)
        def _():
            out_copy(i, held_ref, out_ref, sems).wait()

        if i < HALO_BLOCKS:

            @pl.when(low_ref[i // 2 * 2] < HALO)
            def _():
                part_copy(i, kept_ref, part_ref, sems).wait()


def attend_local(low, ends, qkv):
    vmem = pl.BlockSpec(memory_space=pltpu.VMEM)
    any_space = pl.BlockSpec(memory_space=pl.ANY)
    return pl.pallas_call(
        local_body,
        in_specs=[pl.BlockSpec(memory_space=pltpu.SMEM), vmem, vmem],
        out_specs=[any_space, vmem, any_space],
        out_shape=[
            jax.ShapeDtypeStruct((SPAN, 256), jnp.bfloat16),
            jax.ShapeDtypeStruct((128, 128), jnp.float32),
            jax.ShapeDtypeStruct((HALO_BLOCKS, 2, 2 * TQ, 128), jnp.float32),
        ],
        scratch_shapes=[
            pltpu.VMEM((BLOCKS, TQ, 256), jnp.bfloat16),
            pltpu.VMEM((BLOCKS, 2, 2 * TQ, 128), jnp.float32),
            pltpu.VMEM((MOST_BLOCKS, 2 * TQ, TK), jnp.float32),
            pltpu.SemaphoreType.DMA((2, BLOCKS)),
        ],
        name="attend_local",
    )(low, ends, *in_vmem(qkv))


def halo_body(low_ref, ends_ref, qkv_ref, halo_ref, prev_ref, prev_norm, part_ref, *refs):
    out_ref, *norm_refs = refs[:3]
    held_ref, kept_ref, s_ref, norm_acc, norm_t, sems = refs[3:]
    for i in range(HALO_BLOCKS):

        @pl.when(low_ref[i // 2 * 2] < HALO)
        def _():
            part_copy(i, part_ref, kept_ref, sems).start()

    norm_acc[...] = prev_norm[...]
    rows = lambda j: pl.ds(pl.multiple_of(j * TK, TK), TK)
    keys_at = lambda j: halo_ref[rows(j), 0:128]
    values_at = lambda j: halo_ref[rows(j), 128:256]

    def pair(p, carry):
        pair_blocks = (2 * p, 2 * p + 1)
        j_low = low_ref[2 * p] // TK
        count = HALO // TK - j_low
        for blocks in range(1, HALO // TK + 1):

            @pl.when(count == blocks)
            def _():
                top, total, acc = partial_softmax(
                    [part for i in pair_blocks for part in head_parts(qkv_ref, i)],
                    [positions(i) for i in pair_blocks],
                    j_low,
                    blocks,
                    False,
                    ends_ref,
                    keys_at,
                    values_at,
                    s_ref,
                )
                for i in pair_blocks:
                    part_copy(i, part_ref, kept_ref, sems).wait()
                for n, i in enumerate(pair_blocks):
                    at = slice(2 * n * TQ, 2 * (n + 1) * TQ)
                    own, these = kept_ref[i, 1], top[at] * SCALE
                    most = jnp.maximum(own, these)
                    own, these = jnp.exp(own - most), jnp.exp(these - most)
                    whole = own + total[at] * these
                    keep(held_ref, i, (kept_ref[i, 0] * own + acc[at] * these) / whole)
                    out_copy(i, held_ref, out_ref, sems).start()
                    keep_norm(norm_acc, i, most + jnp.log(whole))

        return carry

    lax.fori_loop(0, HALO_BLOCKS // 2, pair, 0)
    norm_t[...] = jnp.transpose(norm_acc[...])
    for d in range(8):
        norm_refs[d // 4][d % 4] = norm_t[pl.ds(pl.multiple_of(((low_ref[BLOCKS] + d) % 8) * 8, 8), 8)]
    for i in range(HALO_BLOCKS):

        @pl.when(low_ref[i // 2 * 2] < HALO)
        def _():
            out_copy(i, held_ref, out_ref, sems).wait()


def attend_halo(low, ends, qkv, halo, out, norm, part):
    vmem = pl.BlockSpec(memory_space=pltpu.VMEM)
    any_space = pl.BlockSpec(memory_space=pl.ANY)
    return pl.pallas_call(
        halo_body,
        in_specs=[
            pl.BlockSpec(memory_space=pltpu.SMEM),
            vmem,
            vmem,
            vmem,
            any_space,
            vmem,
            any_space,
        ],
        out_specs=[any_space] + [vmem] * 2,
        out_shape=[jax.ShapeDtypeStruct((SPAN, 256), jnp.bfloat16)]
        + [pltpu.VMEM((4, 8, 128), jnp.float32)] * 2,
        scratch_shapes=[
            pltpu.VMEM((HALO_BLOCKS, TQ, 256), jnp.bfloat16),
            pltpu.VMEM((HALO_BLOCKS, 2, 2 * TQ, 128), jnp.float32),
            pltpu.VMEM((HALO // TK, 4 * TQ, TK), jnp.float32),
            pltpu.VMEM((128, 128), jnp.float32),
            pltpu.VMEM((128, 128), jnp.float32),
            pltpu.SemaphoreType.DMA((2, HALO_BLOCKS)),
        ],
        input_output_aliases={4: 0},
        name="attend_halo",
    )(low, ends, *in_vmem(qkv, halo), out, norm, part)


def per_device(queries, keys, values, lengths):
    row = lax.axis_index("z")
    base = lax.axis_index("x") * SPAN
    packed = pack(queries, keys, values).reshape(128, 16, 512)
    moved = lax.all_to_all(packed, PLANE, 0, 0, tiled=True)
    low, ends = bounds(lengths, row[None], base[None])
    qkv = moved.reshape(SPAN, 512)
    halo = lax.ppermute(qkv[SPAN - HALO :, 256:512], "x", [(i, i + 1) for i in range(3)])
    out, norm, part = attend_local(low, ends, qkv)
    out, near, far = attend_halo(low, ends, qkv, halo, out, norm, part)
    back = lax.all_to_all(out.reshape(128, 16, 256), PLANE, 0, 0, tiled=True)
    far = lax.ppermute(far, "z", [(i, (i + 4) % 8) for i in range(8)])
    pairs = [jnp.stack((near[d], far[d])) for d in range(4)]
    for d in range(1, 4):
        pairs[d] = lax.ppermute(pairs[d], "z", [(i, (i + d) % 8) for i in range(8)])
    attended, log_norm = unpack(row[None], back.reshape(ROWS, KV_HEADS, 16, 256), pairs)
    return attended, log_norm


def solution(mesh):
    split = Mesh(mesh.devices.reshape(4, 8, 8, 2), ALL)
    wide = P(None, ALL, None)
    return jax.shard_map(
        per_device,
        mesh=split,
        in_specs=(wide, wide, wide, P()),
        out_specs=(wide, P(("y", "c"), None, ("x", "z"))),
        check_vma=False,
    )
```

```python
import jax
import jax.numpy as jnp
from jax import lax
from jax.experimental import pallas as pl
from jax.experimental.pallas import tpu as pltpu
from jax.sharding import Mesh
from jax.sharding import PartitionSpec as P

HEAD = 128
ROWS = 8
KV_HEADS = 16
HALO = 1024
SPAN = 2048
TQ = 256
TK = 256
MOST_BLOCKS = 5
BLOCKS = SPAN // TQ
HALO_BLOCKS = HALO // TQ
FAR = 1 << 20
LOG2E = 1.4426950408889634
SCALE = HEAD ** (-0.5)
ALL = ("x", "z", "y", "c")
PLANE = ("z", "y", "c")


def in_vmem(*arrays):
    return [pltpu.with_memory_space_constraint(a, pltpu.VMEM) for a in arrays]


def doc_bounds(lengths_ref, row, base, low_ref, ends_ref):
    origin = HALO - base
    slot = lax.broadcasted_iota(jnp.int32, (12, TK), 0) * TK
    slot = slot + lax.broadcasted_iota(jnp.int32, (12, TK), 1)
    end = origin
    low = [origin] * BLOCKS
    after = jnp.full((12, TK), FAR, jnp.int32)
    for n in range(32):
        end = end + lengths_ref[row, n]
        low = [jnp.where(end <= HALO + i * TQ, end, low[i]) for i in range(BLOCKS)]
        after = jnp.minimum(after, jnp.where(slot < end, end, FAR))
    ends_ref[...] = jnp.where(slot < origin, 0, after)
    for i in range(BLOCKS):
        low_ref[i] = low[i]
    low_ref[BLOCKS] = row


def bounds_body(lengths_ref, row_ref, base_ref, low_ref, ends_ref):
    doc_bounds(lengths_ref, row_ref[0], base_ref[0], low_ref, ends_ref)


def bounds(lengths, row, base):
    smem = pl.BlockSpec(memory_space=pltpu.SMEM)
    return pl.pallas_call(
        bounds_body,
        in_specs=[smem] * 3,
        out_specs=[smem, pl.BlockSpec(memory_space=pltpu.VMEM)],
        out_shape=[
            jax.ShapeDtypeStruct((BLOCKS + 1,), jnp.int32),
            pltpu.VMEM((12, TK), jnp.int32),
        ],
        name="doc_bounds",
    )(lengths, row, base)


def pack_body(q_ref, k_ref, v_ref, out_ref, held_ref, sems):
    parts = ((q_ref, 256, 0), (k_ref, 128, 256), (v_ref, 128, 384))
    reads = [
        [
            pltpu.make_async_copy(
                ref.at[:, :, pl.ds(h * width, width)],
                held_ref.at[:, h, :, pl.ds(at, width)],
                sems.at[n, h],
            )
            for n, (ref, width, at) in enumerate(parts)
        ]
        for h in range(KV_HEADS)
    ]
    writes = [
        pltpu.make_async_copy(held_ref.at[:, h], out_ref.at[:, h], sems.at[3, h])
        for h in range(KV_HEADS)
    ]
    for copies in reads:
        for copy in copies:
            copy.start()
    for h in range(KV_HEADS):
        for copy in reads[h]:
            copy.wait()
        writes[h].start()
    for copy in writes:
        copy.wait()


def pack(queries, keys, values):
    return pl.pallas_call(
        pack_body,
        in_specs=[pl.BlockSpec(memory_space=pl.ANY)] * 3,
        out_specs=pl.BlockSpec(memory_space=pl.ANY),
        out_shape=jax.ShapeDtypeStruct((ROWS, KV_HEADS, 16, 512), jnp.bfloat16),
        scratch_shapes=[
            pltpu.VMEM((ROWS, KV_HEADS, 16, 512), jnp.bfloat16),
            pltpu.SemaphoreType.DMA((4, KV_HEADS)),
        ],
        name="pack",
    )(queries, keys, values)


def unpack_body(row_ref, in_ref, *refs):
    *pieces, out_ref, norm_out, norm_ref, sems, norm_sem = refs
    copies = [
        pltpu.make_async_copy(
            in_ref.at[:, h], out_ref.at[:, :, pl.ds(h * 256, 256)], sems.at[h]
        )
        for h in range(KV_HEADS)
    ]
    for copy in copies:
        copy.start()
    rows = lax.broadcasted_iota(jnp.int32, (8, 128), 0)
    for h in range(2):
        for n in range(2):
            at = 2 * h + n
            held = jnp.zeros((8, 128), jnp.float32)
            for d in range(8):
                held = jnp.where(rows == (row_ref[0] + 8 - d) % 8, pieces[d][at : at + 1], held)
            norm_ref[h, :, n * 128 : (n + 1) * 128] = held
    norm_copy = pltpu.make_async_copy(norm_ref, norm_out, norm_sem)
    norm_copy.start()
    norm_copy.wait()
    for copy in copies:
        copy.wait()


def unpack(row, parts, pieces):
    vmem = pl.BlockSpec(memory_space=pltpu.VMEM)
    return pl.pallas_call(
        unpack_body,
        in_specs=[pl.BlockSpec(memory_space=pltpu.SMEM)] + [vmem] * 9,
        out_specs=[pl.BlockSpec(memory_space=pl.ANY)] * 2,
        out_shape=[
            jax.ShapeDtypeStruct((ROWS, 16, 4096), jnp.bfloat16),
            jax.ShapeDtypeStruct((2, ROWS, 256), jnp.float32),
        ],
        scratch_shapes=[
            pltpu.VMEM((2, ROWS, 256), jnp.float32),
            pltpu.SemaphoreType.DMA((KV_HEADS,)),
            pltpu.SemaphoreType.DMA,
        ],
        name="unpack",
    )(row, *in_vmem(parts, *pieces))


def partial_softmax(parts, rows, j_low, blocks, diagonal, ends_ref, keys_at, values_at, s_ref):
    tops, totals, accs = [], [], []
    for p in range(len(parts)):
        at, row, top = slice(p * TQ, (p + 1) * TQ), rows[p // 2], None
        for n in range(blocks):
            s = lax.dot_general(
                parts[p],
                keys_at(j_low + n),
                (((1,), (1,)), ((), ())),
                preferred_element_type=jnp.float32,
            )
            seen = row < ends_ref[pl.ds(j_low + n, 1), :]
            if diagonal and n == blocks - 1:
                key = lax.broadcasted_iota(jnp.int32, (TQ, TK), 1) + (j_low + n) * TK
                seen = seen & (key <= row)
            s = jnp.where(seen, s, -1e30)
            s_ref[n, at] = s
            here = jnp.maximum(s[:, 0:128], s[:, 128:256])
            top = here if top is None else jnp.maximum(top, here)
        tops.append(jnp.broadcast_to(jnp.max(top, axis=1, keepdims=True), top.shape))
    for p in range(len(parts)):
        at, total, acc = slice(p * TQ, (p + 1) * TQ), None, None
        top = jnp.concatenate((tops[p], tops[p]), axis=1)
        for n in range(blocks):
            w = jnp.exp2((s_ref[n, at] - top) * (SCALE * LOG2E))
            part = w[:, 0:128] + w[:, 128:256]
            o = jnp.dot(
                w.astype(jnp.bfloat16), values_at(j_low + n), preferred_element_type=jnp.float32
            )
            total = part if total is None else total + part
            acc = o if acc is None else acc + o
        lead = total.astype(jnp.bfloat16)
        trail = (total - lead.astype(jnp.float32)).astype(jnp.bfloat16)
        totals.append(
            jnp.dot(
                jnp.concatenate((lead, trail), axis=1),
                jnp.ones((256, 128), jnp.bfloat16),
                preferred_element_type=jnp.float32,
            )
        )
        accs.append(acc)
    return tuple(jnp.concatenate(v, axis=0) for v in (tops, totals, accs))


def head_parts(qkv_ref, i):
    q = qkv_ref[pl.ds(pl.multiple_of(i * TQ, TQ), TQ), 0:256]
    return [q[:, 0:128], q[:, 128:256]]


def positions(i):
    return lax.broadcasted_iota(jnp.int32, (TQ, TK), 0) + (HALO + i * TQ)


def out_copy(i, held_ref, out_ref, sems):
    return pltpu.make_async_copy(held_ref.at[i], out_ref.at[pl.ds(i * TQ, TQ)], sems.at[0, i])


def keep(held_ref, i, result):
    result = result.astype(jnp.bfloat16)
    held_ref[i, :, 0:128] = result[0:TQ]
    held_ref[i, :, 128:256] = result[TQ : 2 * TQ]


def norm_lanes(i):
    return [(8 * i + n, slice(n * 128, (n + 1) * 128)) for n in range(4)]


def keep_norm(norm_acc, i, norm):
    lanes = lax.broadcasted_iota(jnp.int32, (128, 128), 1)
    held = norm_acc[...]
    for lane, rows in norm_lanes(i):
        held = jnp.where(lanes == lane, norm[rows], held)
    norm_acc[...] = held


def local_body(
    low_ref, ends_ref, qkv_ref, out_ref, norm_ref, part_ref, held_ref, s_ref, sems
):
    norm_ref[...] = jnp.zeros((128, 128), jnp.float32)
    rows = lambda j: pl.ds(pl.multiple_of(j * TK - HALO, TK), TK)
    keys_at = lambda j: qkv_ref[rows(j), 256:384]
    values_at = lambda j: qkv_ref[rows(j), 384:512]

    def block(i, carry):
        first = pl.multiple_of(i * TQ, TQ)
        j_low = jnp.maximum(low_ref[i], HALO) // TK
        count = (HALO + first) // TK + 1 - j_low
        parts, row = head_parts(qkv_ref, i), positions(i)
        for blocks in range(1, MOST_BLOCKS + 1):

            @pl.when(count == blocks)
            def _():
                top, total, acc = partial_softmax(
                    parts, [row], j_low, blocks, True, ends_ref, keys_at, values_at, s_ref
                )
                result = acc / total
                norm = top * SCALE + jnp.log(total)

                @pl.when(i < HALO_BLOCKS)
                def _():
                    part_ref[i, 0] = result
                    part_ref[i, 1] = norm

                keep(held_ref, i, result)
                keep_norm(norm_ref, i, norm)

        pair_low = low_ref[i // 2 * 2]

        @pl.when(pair_low >= HALO)
        def _():
            out_copy(i, held_ref, out_ref, sems).start()

        return carry

    lax.fori_loop(0, BLOCKS, block, 0)
    for i in range(BLOCKS):

        @pl.when(low_ref[i // 2 * 2] >= HALO)
        def _():
            out_copy(i, held_ref, out_ref, sems).wait()


def attend_local(low, ends, qkv):
    vmem = pl.BlockSpec(memory_space=pltpu.VMEM)
    any_space = pl.BlockSpec(memory_space=pl.ANY)
    return pl.pallas_call(
        local_body,
        in_specs=[pl.BlockSpec(memory_space=pltpu.SMEM), vmem, vmem],
        out_specs=[any_space, vmem, vmem],
        out_shape=[
            jax.ShapeDtypeStruct((SPAN, 256), jnp.bfloat16),
            pltpu.VMEM((128, 128), jnp.float32),
            pltpu.VMEM((HALO_BLOCKS, 2, 2 * TQ, 128), jnp.float32),
        ],
        scratch_shapes=[
            pltpu.VMEM((BLOCKS, TQ, 256), jnp.bfloat16),
            pltpu.VMEM((MOST_BLOCKS, 2 * TQ, TK), jnp.float32),
            pltpu.SemaphoreType.DMA((1, BLOCKS)),
        ],
        name="attend_local",
    )(low, *in_vmem(ends), qkv)


def halo_body(low_ref, ends_ref, qkv_ref, halo_ref, prev_ref, prev_norm, part_ref, *refs):
    out_ref, *norm_refs = refs[:9]
    held_ref, q_ref, s_ref, norm_acc, norm_t, sems, q_sem = refs[9:]
    q_copy = pltpu.make_async_copy(qkv_ref.at[pl.ds(0, HALO), pl.ds(0, 256)], q_ref, q_sem)

    @pl.when(low_ref[0] < HALO)
    def _():
        q_copy.start()

    norm_acc[...] = prev_norm[...]
    rows = lambda j: pl.ds(pl.multiple_of(j * TK, TK), TK)
    keys_at = lambda j: halo_ref[rows(j), 0:128]
    values_at = lambda j: halo_ref[rows(j), 128:256]

    @pl.when(low_ref[0] < HALO)
    def _():
        q_copy.wait()

    def pair(p, carry):
        pair_blocks = (2 * p, 2 * p + 1)
        j_low = low_ref[2 * p] // TK
        count = HALO // TK - j_low
        for blocks in range(1, HALO // TK + 1):

            @pl.when(count == blocks)
            def _():
                top, total, acc = partial_softmax(
                    [part for i in pair_blocks for part in head_parts(q_ref, i)],
                    [positions(i) for i in pair_blocks],
                    j_low,
                    blocks,
                    False,
                    ends_ref,
                    keys_at,
                    values_at,
                    s_ref,
                )
                for n, i in enumerate(pair_blocks):
                    at = slice(2 * n * TQ, 2 * (n + 1) * TQ)
                    own, these = part_ref[i, 1], top[at] * SCALE
                    most = jnp.maximum(own, these)
                    own, these = jnp.exp(own - most), jnp.exp(these - most)
                    whole = own + total[at] * these
                    keep(held_ref, i, (part_ref[i, 0] * own + acc[at] * these) / whole)
                    out_copy(i, held_ref, out_ref, sems).start()
                    keep_norm(norm_acc, i, most + jnp.log(whole))

        return carry

    lax.fori_loop(0, HALO_BLOCKS // 2, pair, 0)
    norm_t[...] = jnp.transpose(norm_acc[...])
    for d in range(8):
        norm_refs[d][...] = norm_t[pl.ds(pl.multiple_of(((low_ref[BLOCKS] + d) % 8) * 8, 8), 8)]
    for i in range(HALO_BLOCKS):

        @pl.when(low_ref[i // 2 * 2] < HALO)
        def _():
            out_copy(i, held_ref, out_ref, sems).wait()


def attend_halo(low, ends, qkv, halo, out, norm, part):
    vmem = pl.BlockSpec(memory_space=pltpu.VMEM)
    any_space = pl.BlockSpec(memory_space=pl.ANY)
    return pl.pallas_call(
        halo_body,
        in_specs=[
            pl.BlockSpec(memory_space=pltpu.SMEM),
            vmem,
            any_space,
            vmem,
            any_space,
            vmem,
            vmem,
        ],
        out_specs=[any_space] + [vmem] * 8,
        out_shape=[jax.ShapeDtypeStruct((SPAN, 256), jnp.bfloat16)]
        + [pltpu.VMEM((8, 128), jnp.float32)] * 8,
        scratch_shapes=[
            pltpu.VMEM((HALO_BLOCKS, TQ, 256), jnp.bfloat16),
            pltpu.VMEM((HALO, 256), jnp.bfloat16),
            pltpu.VMEM((HALO // TK, 4 * TQ, TK), jnp.float32),
            pltpu.VMEM((128, 128), jnp.float32),
            pltpu.VMEM((128, 128), jnp.float32),
            pltpu.SemaphoreType.DMA((1, HALO_BLOCKS)),
            pltpu.SemaphoreType.DMA,
        ],
        input_output_aliases={4: 0},
        name="attend_halo",
    )(low, *in_vmem(ends), qkv, *in_vmem(halo), out, *in_vmem(norm, part))


def per_device(queries, keys, values, lengths):
    row = lax.axis_index("z")
    base = lax.axis_index("x") * SPAN
    packed = pack(queries, keys, values).reshape(128, 16, 512)
    moved = lax.all_to_all(packed, PLANE, 0, 0, tiled=True)
    low, ends = bounds(lengths, row[None], base[None])
    qkv = moved.reshape(SPAN, 512)
    halo = lax.ppermute(qkv[SPAN - HALO :, 256:512], "x", [(i, i + 1) for i in range(3)])
    out, norm, part = attend_local(low, ends, qkv)
    out, *pieces = attend_halo(low, ends, qkv, halo, out, norm, part)
    back = lax.all_to_all(out.reshape(128, 16, 256), PLANE, 0, 0, tiled=True)
    for d in range(1, 8):
        pieces[d] = lax.ppermute(pieces[d], "z", [(i, (i + d) % 8) for i in range(8)])
    attended, log_norm = unpack(row[None], back.reshape(ROWS, KV_HEADS, 16, 256), pieces)
    return attended, log_norm


def solution(mesh):
    split = Mesh(mesh.devices.reshape(4, 8, 8, 2), ALL)
    wide = P(None, ALL, None)
    return jax.shard_map(
        per_device,
        mesh=split,
        in_specs=(wide, wide, wide, P()),
        out_specs=(wide, P(("y", "c"), None, ("x", "z"))),
        check_vma=False,
    )
```
